128 devices in a mesh: gx: 16 (over z_hi, y, core), yz: 8 (over z_lo, x).
Axes of the slice: x: 4, y: 4, z: 4 (z_hi: 2, z_lo: 2; z = z_hi * 2 + z_lo), core: 2. Of those that a mesh axis runs over, the one named last changes fastest.
Arguments:
- spectra: bfloat16 [2, 20, 640, 32, 1024], P(None, None, None, 'gx', 'yz'), may hold values from -6 to 6
- kernel_mesh: float32 [20], replicated, may hold values from 0.02 to 6, as said below
- density: float32 [640, 32, 1024], P('gx', None, 'yz'), may hold values from 0.05 to 1
- local_wave: float32 [640, 32, 1024], P('gx', None, 'yz'), may hold values from 0.15 to 4.8
- wave_density: float32 [640, 32, 1024], P('gx', None, 'yz'), may hold values from -1.2 to 1.2
- wave_gradient: float32 [3, 640, 32, 1024], P(None, 'gx', None, 'yz'), may hold values from -0.6 to 0.6
Outputs:
- potential: float32 [640, 32, 1024], P('gx', None, 'yz')
The draws below stay inside these ranges and needn't reach their ends.
Inputs may be any that keep to these rules, and one draw needn't show every extreme that they name: `kernel_mesh`: strictly increasing; entry 0 is at most 0.1 and entry 19 at least 5.0.
All inputs are finite; a program needn't handle non-finite values.
Results may differ from the reference program's by a relative error of at most 0.0033.
Values sent between devices are 32-bit elements.
No kernel may reach another device: no remote copies, remote signals or barrier semaphores. Data moves between devices by JAX's collectives and lax.ppermute only.
A program may use at most 192 MiB of HBM per device.

```python
import math
import jax
import jax.numpy as jnp
from jax import lax

NX = 640
COMP = 20
NY = 32
NZ = 1024


def draw_kernel_mesh(key, part):
    first_key, last_key, step_key = jax.random.split(key, 3)
    first_point = jax.random.uniform(first_key, (), jnp.float32, 0.02, 0.1)
    last_point = jax.random.uniform(last_key, (), jnp.float32, 5.05, 6.0)
    logs = jax.random.uniform(step_key, (COMP - 1,), jnp.float32, math.log(0.5), math.log(2.0))
    steps_raw = jnp.exp(logs)
    steps_scaled = steps_raw / jnp.sum(steps_raw) * (last_point - first_point)
    return jnp.concatenate([first_point[None], first_point + jnp.cumsum(steps_scaled)])


def steps_of(own_key, shape, shards, low, largest):
    loudness = 1.0
    for position, blocks in shards:
        heights = jax.random.uniform(jax.random.fold_in(jax.random.fold_in(own_key, 6), position), (blocks,), jnp.float32, low / len(shards), largest / len(shards))
        loudness = loudness * jnp.repeat(jnp.exp(heights), shape[position] // blocks).reshape((-1,) + (1,) * (len(shape) - 1 - position))
    return loudness


def centred(own_key, dims, width, most, cuts=(), held_as=jnp.bfloat16):
    array = width * jax.random.normal(own_key, dims, jnp.float32)
    if cuts:
        array = array * steps_of(own_key, dims, cuts, -0.22, 0.18)
    return jnp.clip(array, -most, most).astype(held_as)


def setup_inputs(seed: int = 0) -> dict:
    seeds = jax.random.split(jax.random.key(seed), 7)
    return {
        "spectra": centred(seeds[0], (2, COMP, NX, NY, NZ), 1.0, 6.0, ((3, 16), (4, 8))),
        "kernel_mesh": draw_kernel_mesh(jax.random.fold_in(seeds[6], 71), 0),
        "density": jnp.clip(jnp.exp(math.log(1.0) - 2.9957323 * jax.random.uniform(seeds[2], (NX, NY, NZ), jnp.float32) ** steps_of(seeds[2], (NX, NY, NZ), ((0, 16), (2, 8)), -0.2, 0.2)), 0.05, 1.0),
        "local_wave": jnp.clip(0.15 + 4.65 * jax.random.uniform(seeds[3], (NX, NY, NZ), jnp.float32) ** steps_of(seeds[3], (NX, NY, NZ), ((0, 16), (2, 8)), -0.2, 0.2), 0.15, 4.8),
        "wave_density": centred(seeds[4], (NX, NY, NZ), 0.2, 1.2, ((0, 16), (2, 8)), jnp.float32),
        "wave_gradient": centred(seeds[5], (3, NX, NY, NZ), 0.1, 0.6, ((1, 16), (3, 8)), jnp.float32),
    }


def dft_tables(length):
    rows_index = lax.broadcasted_iota(jnp.int32, (length, length), 0)
    cols_index = lax.broadcasted_iota(jnp.int32, (length, length), 1)
    phases = rows_index * cols_index % length
    angles = phases.astype(jnp.float32) * (2.0 * math.pi / length)
    return jnp.stack([jnp.cos(angles), -jnp.sin(angles)]).astype(jnp.bfloat16)

def spline_second(kernel_mesh):
    points = kernel_mesh.shape[0]
    spacing = kernel_mesh[1:] - kernel_mesh[:-1]
    identity = jnp.eye(points, dtype=jnp.float32)
    right_side = (identity[2:] - identity[1:-1]) / spacing[1:, None] - (identity[1:-1] - identity[:-2]) / spacing[:-1, None]
    zero_entry = jnp.zeros((1,), jnp.float32)
    lower_band = jnp.concatenate([zero_entry, spacing[1:-1] / 6.0])
    main_band = (spacing[:-1] + spacing[1:]) / 3.0
    upper_band = jnp.concatenate([spacing[1:-1] / 6.0, zero_entry])
    interior = lax.linalg.tridiagonal_solve(lower_band, main_band, upper_band, right_side)
    border = jnp.zeros((1, points), jnp.float32)
    return jnp.concatenate([border, interior, border])

def basis_terms(weight_a, weight_b, span_width, lower_hot, upper_hot, second_lower, second_upper):
    basis_value = weight_a * lower_hot + weight_b * upper_hot + (weight_a * weight_a * weight_a - weight_a) * span_width * span_width / 6.0 * second_lower + (weight_b * weight_b * weight_b - weight_b) * span_width * span_width / 6.0 * second_upper
    basis_slope = (upper_hot - lower_hot) / span_width - (3.0 * weight_a * weight_a - 1.0) * span_width / 6.0 * second_lower + (3.0 * weight_b * weight_b - 1.0) * span_width / 6.0 * second_upper
    return (basis_value, basis_slope)

def reference(spectra, kernel_mesh, density, local_wave, wave_density, wave_gradient):
    tables = dft_tables(NX).astype(jnp.float32)
    second = spline_second(kernel_mesh)
    points = kernel_mesh.shape[0]
    interval = jnp.zeros(local_wave.shape, jnp.int32)
    for index in range(1, points - 1):
        interval = interval + (local_wave >= kernel_mesh[index]).astype(jnp.int32)
    lower_point = jnp.take(kernel_mesh, interval)
    finish_point = jnp.take(kernel_mesh, interval + 1)
    span_width = finish_point - lower_point
    weight_a = (finish_point - local_wave) / span_width
    weight_b = (local_wave - lower_point) / span_width

    def accumulate(carry, alpha):
        sum_value, sum_slope = carry
        spectrum = lax.dynamic_index_in_dim(spectra, alpha, 1, keepdims=False).astype(jnp.float32)
        summed = jnp.einsum('pkyz,pkx->xyz', spectrum, tables, precision=lax.Precision.HIGHEST)
        values = summed * NX ** (-0.5)
        lower_hot = (interval == alpha).astype(jnp.float32)
        upper_hot = (interval + 1 == alpha).astype(jnp.float32)
        column = lax.dynamic_index_in_dim(second, alpha, 1, keepdims=False)
        second_lower = jnp.take(column, interval)
        second_upper = jnp.take(column, interval + 1)
        basis_value, basis_slope = basis_terms(weight_a, weight_b, span_width, lower_hot, upper_hot, second_lower, second_upper)
        return ((sum_value + values * basis_value, sum_slope + values * basis_slope), None)
    blank_field = jnp.zeros(local_wave.shape, jnp.float32)
    (sum_value, sum_slope), unused = lax.scan(accumulate, (blank_field, blank_field), jnp.arange(points, dtype=jnp.int32))
    local_term = sum_value + density * wave_density * sum_slope
    grad_scale = density * sum_slope
    divergence = jnp.zeros(local_wave.shape, jnp.float32)
    for axis_index in range(3):
        flux = grad_scale * wave_gradient[axis_index]
        divergence = divergence + 0.5 * (jnp.roll(flux, -1, axis_index) - jnp.roll(flux, 1, axis_index))
    return local_term - divergence
```

```python
import math

import jax
import jax.numpy as jnp
import numpy as np
from jax import lax
from jax.experimental import pallas as pl
from jax.experimental.pallas import tpu as pltpu
from jax.sharding import PartitionSpec as P

LANES = 128
COMPS_PER_STEP = 2
BLOCKS_PER_STEP = 2
IH, LOW, INV, MESH, ROWS = 0, 20, 40, 60, 80


def half_tables(length):
    half = length // 2
    cells = np.arange(half)[:, None]
    tables = []
    for parity in range(2):
        waves = 2 * np.arange(half)[None, :] + parity
        angles = 2.0 * math.pi * (waves * cells % length) / length
        tables.append(np.concatenate([np.cos(angles), -np.sin(angles)], axis=1))
    return np.stack(tables).astype(jnp.bfloat16)


def spline_table(mesh_ref, table_ref):
    points = mesh_ref.shape[0]
    tile = (8, LANES)
    mesh = [jnp.full(tile, mesh_ref[j], jnp.float32) for j in range(points)]
    steps = [mesh[j + 1] - mesh[j] for j in range(points - 1)]
    for j in range(points):
        table_ref[MESH + j] = mesh[j]
    for j in range(points - 1):
        table_ref[IH + j] = 1.0 / steps[j]
    low = jnp.zeros(tile, jnp.float32)
    for j in range(1, points - 1):
        pivot = (steps[j - 1] + steps[j]) / 3.0 - low * (steps[j - 1] / 6.0)
        inverse = 1.0 / pivot
        table_ref[LOW + j] = low
        table_ref[INV + j] = inverse
        low = (steps[j] / 6.0) * inverse
    table_ref[LOW + points - 1] = low


def transform_kernel(mesh_ref, tables_ref, spectra_ref, comp_ref, table_ref, scratch):
    @pl.when(pl.program_id(0) == 0)
    def _():
        spline_table(mesh_ref, table_ref)

    per_step = spectra_ref.shape[1]
    length = comp_ref.shape[2]
    half = length // 2
    for c in range(per_step):
        for p in range(2):
            scratch[c, p] = spectra_ref[p, c].astype(jnp.float32)
        parts = []
        for parity in range(2):
            operand = jnp.concatenate(
                [
                    jnp.concatenate(
                        [
                            scratch[c, p, pl.ds(2 * parity + y, half, stride=4), :].astype(jnp.bfloat16)
                            for y in range(2)
                        ],
                        axis=1,
                    )
                    for p in range(2)
                ],
                axis=0,
            )
            parts.append(jnp.dot(tables_ref[parity], operand, preferred_element_type=jnp.float32))
        total, difference = parts[0] + parts[1], parts[0] - parts[1]
        for y in range(2):
            comp_ref[c, y, :half, :] = total[:, y * LANES : (y + 1) * LANES]
            comp_ref[c, y, half:, :] = difference[:, y * LANES : (y + 1) * LANES]


def transform(spectra, kernel_mesh):
    comps, length = spectra.shape[1], spectra.shape[2]
    per_step = COMPS_PER_STEP
    tables = jnp.asarray(half_tables(length))
    flat = spectra.reshape(2, comps, 2 * length, LANES)
    return pl.pallas_call(
        transform_kernel,
        grid=(comps // per_step,),
        in_specs=[
            pl.BlockSpec(memory_space=pltpu.SMEM),
            pl.BlockSpec((2, length // 2, length), lambda i: (0, 0, 0)),
            pl.BlockSpec((2, per_step, 2 * length, LANES), lambda i: (0, i, 0, 0)),
        ],
        out_specs=[
            pl.BlockSpec((per_step, 2, length, LANES), lambda i: (i, 0, 0, 0)),
            pl.BlockSpec((ROWS, 8, LANES), lambda i: (0, 0, 0)),
        ],
        out_shape=[
            jax.ShapeDtypeStruct((comps, 2, length, LANES), jnp.float32),
            jax.ShapeDtypeStruct((ROWS, 8, LANES), jnp.float32),
        ],
        scratch_shapes=[pltpu.VMEM((per_step, 2, 2 * length, LANES), jnp.float32)],
        cost_estimate=pl.CostEstimate(
            flops=4 * comps * length * length * LANES,
            bytes_accessed=12 * comps * length * 2 * LANES,
            transcendentals=0,
        ),
        name="transform",
    )(kernel_mesh, tables, flat)


def evaluate(comp, table, wave):
    points = 20
    step, before = None, None
    forward = [None] * points
    for j in range(points - 1):
        step = (comp(j + 1) - comp(j)) * table(IH + j)
        if j >= 1:
            right = step - before
            forward[j] = right if j == 1 else right - table(LOW + j) * forward[j - 1]
        before = step
    second = [None] * points
    second[points - 1] = jnp.zeros_like(wave)
    second[0] = jnp.zeros_like(wave)
    for j in range(points - 2, 0, -1):
        second[j] = forward[j] * table(INV + j)
        if j < points - 2:
            second[j] = second[j] - table(LOW + j + 1) * second[j + 1]

    def pick(node):
        held = [node(points - 4 + i) for i in range(4)]
        for first in range(points - 7, 0, -3):
            below = wave < table(MESH + first + 3)
            held = [jnp.where(below, node(first + i), held[i]) for i in range(4)]
        below = wave < table(MESH + 1)
        return [jnp.where(below, node(min(i, 1)), held[i]) for i in range(4)]

    def ends(four, past_one, past_two):
        lower = jnp.where(past_two, four[2], jnp.where(past_one, four[1], four[0]))
        upper = jnp.where(past_two, four[3], jnp.where(past_one, four[2], four[1]))
        return lower, upper

    points_four = pick(lambda j: table(MESH + j))
    past_one, past_two = wave >= points_four[1], wave >= points_four[2]
    low, high = ends(points_four, past_one, past_two)
    comp_low, comp_high = ends(pick(comp), past_one, past_two)
    second_low, second_high = ends(pick(lambda j: second[j]), past_one, past_two)
    width = high - low
    inverse = 1.0 / width
    a = (high - wave) * inverse
    b = (wave - low) * inverse
    sixth = width * (1.0 / 6.0)
    a2, b2 = a * a, b * b
    value = a * comp_low + b * comp_high + (
        (a2 - 1.0) * a * second_low + (b2 - 1.0) * b * second_high
    ) * (width * sixth)
    slope = (comp_high - comp_low) * inverse + (
        (3.0 * b2 - 1.0) * second_high - (3.0 * a2 - 1.0) * second_low
    ) * sixth
    return value, slope


def spline_kernel(scale, table_ref, comp_ref, wave_ref, out_ref):
    blocks, width = wave_ref.shape[0], wave_ref.shape[2]
    count = out_ref.shape[0]
    tiles = width // 8
    step = pl.program_id(0)
    for k in range(blocks):
        block = step * blocks + k
        for y in range(2):
            value, slope = evaluate(
                lambda j: comp_ref[j, y, k * width : (k + 1) * width, :].reshape(tiles, 8, LANES),
                lambda j: table_ref[j],
                wave_ref[k, y].reshape(tiles, 8, LANES),
            )
            value = (value * scale).reshape(width, LANES)
            slope = (slope * scale).reshape(width, LANES)
            out_ref[block, y * width : (y + 1) * width, :] = value
            out_ref[block, (2 + y) * width : (3 + y) * width, :] = slope
            following = lax.rem(block + 1, count)
            previous = lax.rem(block + count - 1, count)
            out_ref[following, 4 * width + y : 4 * width + y + 1, :] = slope[width - 1 :]
            out_ref[previous, 4 * width + 2 + y : 4 * width + 3 + y, :] = slope[:1]
            out_ref[block, 4 * width + 4 + 2 * y : 4 * width + 6 + 2 * y, :] = slope[:2]


def splines(comp, table, wave):
    count, width = wave.shape[0], wave.shape[2]
    comps, length = comp.shape[0], comp.shape[2]
    blocks = BLOCKS_PER_STEP
    message = 4 * width + 8
    import functools

    return pl.pallas_call(
        functools.partial(spline_kernel, length ** (-0.5)),
        grid=(count // blocks,),
        in_specs=[
            pl.BlockSpec((ROWS, 8, LANES), lambda i: (0, 0, 0)),
            pl.BlockSpec((comps, 2, blocks * width, LANES), lambda i: (0, 0, i, 0)),
            pl.BlockSpec((blocks, 2, width, LANES), lambda i: (i, 0, 0, 0)),
        ],
        out_specs=pl.BlockSpec((count, message, LANES), lambda i: (0, 0, 0)),
        out_shape=jax.ShapeDtypeStruct((count, message, LANES), jnp.float32),
        name="splines",
    )(table, comp, wave)


def neighbours(axis):
    count = lax.axis_size(axis)
    forward = [(i, (i + 1) % count) for i in range(count)]
    return forward, [(target, source) for source, target in forward]


def shards(spectra, kernel_mesh, density, local_wave, wave_density, wave_gradient):
    width, rows = density.shape[0], density.shape[1]
    count = lax.axis_size("gx")
    wave = local_wave.reshape(width, count, 2, LANES).transpose(1, 2, 0, 3)
    wave = lax.all_to_all(wave, "gx", 0, 0, tiled=True)
    comp, table = transform(spectra, kernel_mesh)
    sent = splines(comp, table, wave)
    got = lax.all_to_all(sent, "gx", 0, 0, tiled=True)

    forward, backward = neighbours("gx")
    push = density * wave_gradient[0]
    push_low = lax.ppermute(push[-1:], "gx", forward)
    push_high = lax.ppermute(push[:1], "gx", backward)

    def field(at):
        part = got[:, at * width : (at + 2) * width].reshape(rows, width, LANES)
        return part.transpose(1, 0, 2)

    sum_value, sum_slope = field(0), field(2)
    edge = got[:, 4 * width : 4 * width + 4].reshape(count, 2, 2, LANES).transpose(1, 0, 2, 3)
    edge = edge.reshape(2, rows, LANES)
    local_term = sum_value + density * wave_density * sum_slope
    grad_scale = density * sum_slope
    flux_first = jnp.concatenate([push_low * edge[:1], push * sum_slope, push_high * edge[1:]], axis=0)
    flux_second = grad_scale * wave_gradient[1]
    flux_third = grad_scale * wave_gradient[2]
    forward, backward = neighbours("yz")
    third_low = lax.ppermute(flux_third[:, :, -1], "yz", forward)
    third_high = lax.ppermute(flux_third[:, :, 0], "yz", backward)
    padded = jnp.concatenate([third_low[:, :, None], flux_third, third_high[:, :, None]], axis=2)
    divergence = 0.5 * (flux_first[2:] - flux_first[:-2])
    divergence = divergence + 0.5 * (jnp.roll(flux_second, -1, 1) - jnp.roll(flux_second, 1, 1))
    divergence = divergence + 0.5 * (padded[:, :, 2:] - padded[:, :, :-2])
    return local_term - divergence


def solution(mesh):
    return jax.shard_map(
        shards,
        mesh=mesh,
        in_specs=(
            P(None, None, None, "gx", "yz"),
            P(),
            P("gx", None, "yz"),
            P("gx", None, "yz"),
            P("gx", None, "yz"),
            P(None, "gx", None, "yz"),
        ),
        out_specs=P("gx", None, "yz"),
        check_vma=False,
    )
```

```python
import functools
import math

import jax
import jax.numpy as jnp
import numpy as np
from jax import lax
from jax.experimental import pallas as pl
from jax.experimental.pallas import tpu as pltpu
from jax.sharding import PartitionSpec as P

LANES = 128
POINTS = 20
GROUP = 4
SLICES = 4
IH, LOW, INV, ROWS = 0, 20, 40, 60


def in_hbm(array):
    return pltpu.with_memory_space_constraint(array, pltpu.HBM)


def half_tables(length):
    half = length // 2
    cells = np.arange(half)[:, None]
    tables = []
    for parity in range(2):
        waves = 2 * np.arange(half)[None, :] + parity
        angles = 2.0 * math.pi * (waves * cells % length) / length
        tables.append(np.concatenate([np.cos(angles), -np.sin(angles)], axis=1))
    return np.stack(tables).astype(jnp.bfloat16)


def spline_table(mesh_ref, table_ref):
    tile = (8, LANES)
    mesh = [jnp.full(tile, mesh_ref[j], jnp.float32) for j in range(POINTS)]
    steps = [mesh[j + 1] - mesh[j] for j in range(POINTS - 1)]
    for j in range(POINTS - 1):
        table_ref[IH + j] = 1.0 / steps[j]
    low = jnp.zeros(tile, jnp.float32)
    for j in range(1, POINTS - 1):
        pivot = (steps[j - 1] + steps[j]) / 3.0 - low * (steps[j - 1] / 6.0)
        inverse = 1.0 / pivot
        table_ref[LOW + j] = low
        table_ref[INV + j] = inverse
        low = (steps[j] / 6.0) * inverse
    table_ref[LOW + POINTS - 1] = low


def transform_kernel(mesh_ref, tables_hbm, spectra_ref, comp_ref, table_out, tables_ref, held, wide, done, table_ref, arrived, left):
    length = comp_ref.shape[1]
    half = length // 2
    groups = POINTS // GROUP

    def copy(c):
        return pltpu.make_async_copy(spectra_ref.at[:, c], held.at[c], arrived.at[c])

    def store(g, slot):
        return pltpu.make_async_copy(done.at[slot], comp_ref.at[pl.ds(g * (2 * GROUP), 2 * GROUP)], left.at[slot])

    tables_copy = pltpu.make_async_copy(tables_hbm, tables_ref, left.at[3])
    copy(0).start()
    tables_copy.start()
    for c in range(1, POINTS):
        copy(c).start()
    spline_table(mesh_ref, table_ref)
    table_copy = pltpu.make_async_copy(table_ref, table_out, left.at[2])
    table_copy.start()
    tables_copy.wait()

    def group(g, carry):
        slot = lax.rem(g, 2)

        @pl.when(g >= 2)
        def _():
            store(g - 2, slot).wait()

        for i in range(GROUP):
            copy(g * GROUP + i).wait()
        for i in range(GROUP):
            c = g * GROUP + i
            for p in range(2):
                wide[i, p] = held[c, p].astype(jnp.float32)
            parts = []
            for parity in range(2):
                operand = jnp.concatenate(
                    [
                        jnp.concatenate(
                            [
                                wide[i, p, pl.ds(2 * parity + y, half, stride=4), :].astype(jnp.bfloat16)
                                for y in range(2)
                            ],
                            axis=1,
                        )
                        for p in range(2)
                    ],
                    axis=0,
                )
                parts.append(jnp.dot(tables_ref[parity], operand, preferred_element_type=jnp.float32))
            total, difference = parts[0] + parts[1], parts[0] - parts[1]
            for y in range(2):
                done[slot, 2 * i + y, :half, :] = total[:, y * LANES : (y + 1) * LANES]
                done[slot, 2 * i + y, half:, :] = difference[:, y * LANES : (y + 1) * LANES]
        store(g, slot).start()
        return carry

    lax.fori_loop(0, groups, group, 0)
    for g in range(groups - 2, groups):
        store(g, g % 2).wait()
    table_copy.wait()


def transform(spectra, kernel_mesh):
    comps, length = spectra.shape[1], spectra.shape[2]
    tables = jnp.asarray(half_tables(length))
    flat = spectra.reshape(2, comps, 2 * length, LANES)
    return pl.pallas_call(
        transform_kernel,
        in_specs=[
            pl.BlockSpec(memory_space=pltpu.SMEM),
            pl.BlockSpec(memory_space=pltpu.HBM),
            pl.BlockSpec(memory_space=pltpu.HBM),
        ],
        out_specs=[pl.BlockSpec(memory_space=pltpu.HBM), pl.BlockSpec(memory_space=pltpu.HBM)],
        out_shape=[
            pltpu.HBM((2 * comps, length, LANES), jnp.float32),
            pltpu.HBM((ROWS, 8, LANES), jnp.float32),
        ],
        scratch_shapes=[
            pltpu.VMEM((2, length // 2, length), jnp.bfloat16),
            pltpu.VMEM((comps, 2, 2 * length, LANES), jnp.bfloat16),
            pltpu.VMEM((GROUP, 2, 2 * length, LANES), jnp.float32),
            pltpu.VMEM((2, 2 * GROUP, length, LANES), jnp.float32),
            pltpu.VMEM((ROWS, 8, LANES), jnp.float32),
            pltpu.SemaphoreType.DMA((comps,)),
            pltpu.SemaphoreType.DMA((4,)),
        ],
        compiler_params=pltpu.CompilerParams(vmem_limit_bytes=40 * 1024 * 1024),
        cost_estimate=pl.CostEstimate(
            flops=4 * comps * length * length * LANES,
            bytes_accessed=12 * comps * length * 2 * LANES,
            transcendentals=0,
        ),
        name="transform",
    )(kernel_mesh, in_hbm(tables), in_hbm(flat))


def solve(comp, table):
    before = (comp(1) - comp(0)) * table(IH)
    forward = [None] * POINTS
    for j in range(1, POINTS - 1):
        step = (comp(j + 1) - comp(j)) * table(IH + j)
        forward[j] = step - before
        if j > 1:
            forward[j] = forward[j] - table(LOW + j) * forward[j - 1]
        before = step
    second = [None] * POINTS
    for j in range(POINTS - 2, 0, -1):
        second[j] = forward[j] * table(INV + j)
        if j < POINTS - 2:
            second[j] = second[j] - table(LOW + j + 1) * second[j + 1]
    second[0] = second[POINTS - 1] = jnp.zeros_like(before)
    return second


def evaluate(comp, second, mesh, wave):
    def pick(node):
        held = [node(POINTS - 4 + i) for i in range(4)]
        for first in range(POINTS - 7, 0, -3):
            below = wave < mesh(first + 3)
            held = [jnp.where(below, node(first + i), held[i]) for i in range(4)]
        below = wave < mesh(1)
        return [jnp.where(below, node(min(i, 1)), held[i]) for i in range(4)]

    def ends(four, past_one, past_two):
        lower = jnp.where(past_two, four[2], jnp.where(past_one, four[1], four[0]))
        upper = jnp.where(past_two, four[3], jnp.where(past_one, four[2], four[1]))
        return lower, upper

    points_four = pick(mesh)
    past_one, past_two = wave >= points_four[1], wave >= points_four[2]
    low, high = ends(points_four, past_one, past_two)
    comp_low, comp_high = ends(pick(comp), past_one, past_two)
    second_low, second_high = ends(pick(second), past_one, past_two)
    width = high - low
    inverse = 1.0 / width
    a = (high - wave) * inverse
    b = (wave - low) * inverse
    sixth = width * (1.0 / 6.0)
    a2, b2 = a * a, b * b
    value = a * comp_low + b * comp_high + (
        (a2 - 1.0) * a * second_low + (b2 - 1.0) * b * second_high
    ) * (width * sixth)
    slope = (comp_high - comp_low) * inverse + (
        (3.0 * b2 - 1.0) * second_high - (3.0 * a2 - 1.0) * second_low
    ) * sixth
    return value, slope


def spline_kernel(scale, mesh_ref, table_ref, wave_ref, comp_ref, out_hbm, order_ref, out_ref, held, arrived, left):
    count, width = wave_ref.shape[0], wave_ref.shape[2]
    tiles = width // 8
    part = 2 * width + 4

    def copy(block):
        rows = pl.ds(pl.multiple_of(block * width, 8), width)
        return pltpu.make_async_copy(comp_ref.at[:, rows], held.at[block], arrived.at[block])

    def store(block):
        return pltpu.make_async_copy(out_ref.at[block], out_hbm.at[block], left.at[block])

    for block in range(count):
        copy(block).start()
    order_ref[...] = jnp.zeros_like(order_ref)
    mesh = [jnp.full((8, LANES), mesh_ref[j], jnp.float32) for j in range(POINTS)]

    def body(block, carry):
        following = lax.rem(block + 1, count)
        previous = lax.rem(block + count - 1, count)
        copy(block).wait()
        slopes = []
        for y in range(2):
            wave = wave_ref[block, y].reshape(tiles, 8, LANES)
            comp = lambda j: held[block, 2 * j + y].reshape(tiles, 8, LANES)
            second = solve(comp, lambda j: table_ref[j])
            value, slope = evaluate(comp, lambda j: second[j], lambda j: mesh[j], wave)
            value = (value * scale).reshape(width, LANES)
            slope = (slope * scale).reshape(width, LANES)
            out_ref[block, y * part : y * part + width, :] = value
            out_ref[block, y * part + width : y * part + 2 * width, :] = slope
            at = y * part + 2 * width
            out_ref[following, at : at + 1, :] = slope[width - 1 :]
            out_ref[previous, at + 1 : at + 2, :] = slope[:1]
            slopes.append(slope)
        slopes.append(jnp.zeros((LANES - 2 * width, LANES), jnp.float32))
        turned = jnp.concatenate(slopes, axis=0).T
        for side, edge in enumerate((turned[:1], turned[LANES - 1 :])):
            out_ref[block, 2 * width + 2 + side : 2 * width + 3 + side, :] = edge
            at = part + 2 * width + 2 + side
            out_ref[block, at : at + 1, :] = pltpu.roll(edge, LANES - width, 1)

        @pl.when(block >= 2)
        def _():
            store(block - 1).start()

        return carry

    lax.fori_loop(0, count, body, 0)
    store(0).start()
    store(count - 1).start()
    for block in range(count):
        store(block).wait()


def splines(kernel_mesh, comp, table, wave):
    count, width = wave.shape[0], wave.shape[2]
    planes, length = comp.shape[0], comp.shape[1]
    vmem = pl.BlockSpec(memory_space=pltpu.VMEM)
    hbm = pl.BlockSpec(memory_space=pltpu.HBM)
    message = (count, 4 * width + 8, LANES)
    return pl.pallas_call(
        functools.partial(spline_kernel, length ** (-0.5)),
        in_specs=[pl.BlockSpec(memory_space=pltpu.SMEM), vmem, vmem, hbm],
        out_specs=[hbm, vmem],
        out_shape=[pltpu.HBM(message, jnp.float32), jax.ShapeDtypeStruct((8, LANES), jnp.float32)],
        scratch_shapes=[
            pltpu.VMEM(message, jnp.float32),
            pltpu.VMEM((count, planes, width, LANES), jnp.float32),
            pltpu.SemaphoreType.DMA((count,)),
            pltpu.SemaphoreType.DMA((count,)),
        ],
        compiler_params=pltpu.CompilerParams(vmem_limit_bytes=28 * 1024 * 1024),
        name="splines",
    )(kernel_mesh, table, wave, in_hbm(comp))


def edges_kernel(order_ref, density_ref, gradient_ref, push_ref, weight_ref, density, first, third, arrived):
    width, rows = density_ref.shape[0], density_ref.shape[1]
    copies = [
        pltpu.make_async_copy(density_ref, density, arrived.at[0]),
        pltpu.make_async_copy(gradient_ref.at[2], third, arrived.at[1]),
        pltpu.make_async_copy(gradient_ref.at[0, 0], first.at[0], arrived.at[2]),
        pltpu.make_async_copy(gradient_ref.at[0, width - 1], first.at[1], arrived.at[3]),
    ]
    for copy in copies:
        copy.start()
    for copy in copies:
        copy.wait()
    push_ref[0] = density[0] * first[0]
    push_ref[1] = density[width - 1] * first[1]
    lane = lax.broadcasted_iota(jnp.int32, (rows, LANES), 1)
    low = order_ref[:1] + jnp.zeros((rows, LANES), jnp.float32)
    high = low
    for x in range(width):
        product = density[x] * third[x]
        low = jnp.where(lane == x, product[:, :1], low)
        high = jnp.where(lane == x, product[:, LANES - 1 :], high)
    weight_ref[0] = low
    weight_ref[1] = high


def edges(order, density, gradient):
    rows = density.shape[1]
    vmem, hbm = pl.BlockSpec(memory_space=pltpu.VMEM), pl.BlockSpec(memory_space=pltpu.HBM)
    face = jax.ShapeDtypeStruct((2, rows, LANES), jnp.float32)
    return pl.pallas_call(
        edges_kernel,
        in_specs=[vmem, hbm, hbm],
        out_specs=[vmem, vmem],
        out_shape=[face, face],
        scratch_shapes=[
            pltpu.VMEM(density.shape, jnp.float32),
            pltpu.VMEM((2, rows, LANES), jnp.float32),
            pltpu.VMEM(density.shape, jnp.float32),
            pltpu.SemaphoreType.DMA((4,)),
        ],
        compiler_params=pltpu.CompilerParams(vmem_limit_bytes=8 * 1024 * 1024),
        name="edges",
    )(order, in_hbm(density), in_hbm(gradient))


def faces_kernel(width, got_ref, weight_ref, out_ref):
    part, rows = 2 * width + 4, weight_ref.shape[1]
    for side in range(2):
        out_ref[side] = got_ref[pl.ds(2 * width + 2 + side, rows, stride=part), :] * weight_ref[side]


def faces(got, weight, width):
    vmem = pl.BlockSpec(memory_space=pltpu.VMEM)
    return pl.pallas_call(
        functools.partial(faces_kernel, width),
        in_specs=[vmem, vmem],
        out_specs=vmem,
        out_shape=jax.ShapeDtypeStruct(weight.shape, jnp.float32),
        compiler_params=pltpu.CompilerParams(vmem_limit_bytes=8 * 1024 * 1024),
        name="faces",
    )(got, weight)


def inner_kernel(got_ref, push_ref, density_ref, rate_ref, gradient_ref, result, density, rate, gradient, arrived):
    width, rows = density_ref.shape[0], density_ref.shape[1]
    part = 2 * width + 4
    share = width // SLICES

    def copies(n):
        at = pl.ds(n * share, share)
        return [
            pltpu.make_async_copy(density_ref.at[at], density.at[at], arrived.at[n, 0]),
            pltpu.make_async_copy(rate_ref.at[at], rate.at[at], arrived.at[n, 1]),
            pltpu.make_async_copy(gradient_ref.at[:, at], gradient.at[:, at], arrived.at[n, 2]),
        ]

    for n in range(SLICES):
        for copy in copies(n):
            copy.start()

    def field(at):
        return got_ref[pl.ds(at, rows, stride=part), :]

    lane = lax.broadcasted_iota(jnp.int32, (rows, LANES), 1)
    ready = 0
    slope = [None] * width
    first = [None] * width
    for x in range(-1, width):
        ahead = x + 1
        if ahead < width:
            if ahead % share == 0:
                for copy in copies(ahead // share):
                    copy.wait()
            slope[ahead] = field(width + ahead) * density[ahead]
            first[ahead] = slope[ahead] * gradient[0, ahead]
        if x < 0:
            continue
        below = first[x - 1] if x > 0 else field(2 * width) * push_ref[0]
        above = first[x + 1] if x + 1 < width else field(2 * width + 1) * push_ref[1]
        second = slope[x] * gradient[1, x]
        third = slope[x] * gradient[2, x]
        beyond = jnp.where(lane == LANES - 1, 0.0, pltpu.roll(third, LANES - 1, 1))
        behind = jnp.where(lane == 0, 0.0, pltpu.roll(third, 1, 1))
        divergence = (above - below) + (beyond - behind)
        divergence = divergence + (pltpu.roll(second, rows - 1, 0) - pltpu.roll(second, 1, 0))
        result[x] = field(x) + rate[x] * slope[x] - 0.5 * divergence


def inner(got, push, density, rate, gradient):
    vmem, hbm = pl.BlockSpec(memory_space=pltpu.VMEM), pl.BlockSpec(memory_space=pltpu.HBM)
    return pl.pallas_call(
        inner_kernel,
        in_specs=[vmem, vmem, hbm, hbm, hbm],
        out_specs=vmem,
        out_shape=jax.ShapeDtypeStruct(density.shape, jnp.float32),
        scratch_shapes=[
            pltpu.VMEM(density.shape, jnp.float32),
            pltpu.VMEM(density.shape, jnp.float32),
            pltpu.VMEM(gradient.shape, jnp.float32),
            pltpu.SemaphoreType.DMA((SLICES, 3)),
        ],
        compiler_params=pltpu.CompilerParams(vmem_limit_bytes=16 * 1024 * 1024),
        name="inner",
    )(got, push, in_hbm(density), in_hbm(rate), in_hbm(gradient))


def outer_kernel(part_ref, low_ref, high_ref, out_hbm, out_ref, left):
    width, rows = part_ref.shape[0], part_ref.shape[1]
    share = width // SLICES
    lane = lax.broadcasted_iota(jnp.int32, (rows, LANES), 1)

    def store(n):
        at = pl.ds(n * share, share)
        return pltpu.make_async_copy(out_ref.at[at], out_hbm.at[at], left.at[n])

    for x in range(width):
        high = jnp.where(lane == LANES - 1, high_ref[:, x : x + 1], 0.0)
        flux = jnp.where(lane == 0, low_ref[:, x : x + 1], 0.0) - high
        out_ref[x] = part_ref[x] + 0.5 * flux
        if (x + 1) % share == 0:
            store(x // share).start()
    for n in range(SLICES):
        store(n).wait()


def outer(part, low, high):
    vmem, hbm = pl.BlockSpec(memory_space=pltpu.VMEM), pl.BlockSpec(memory_space=pltpu.HBM)
    return pl.pallas_call(
        outer_kernel,
        in_specs=[vmem] * 3,
        out_specs=hbm,
        out_shape=jax.ShapeDtypeStruct(part.shape, jnp.float32),
        scratch_shapes=[pltpu.VMEM(part.shape, jnp.float32), pltpu.SemaphoreType.DMA((SLICES,))],
        compiler_params=pltpu.CompilerParams(vmem_limit_bytes=8 * 1024 * 1024),
        name="outer",
    )(part, low, high)


def neighbours(axis):
    count = lax.axis_size(axis)
    forward = [(i, (i + 1) % count) for i in range(count)]
    return forward, [(target, source) for source, target in forward]


def shards(spectra, kernel_mesh, density, local_wave, wave_density, wave_gradient):
    width, rows = density.shape[0], density.shape[1]
    count = lax.axis_size("gx")
    wave = local_wave.reshape(width, count, 2, LANES).transpose(1, 2, 0, 3)
    wave = lax.all_to_all(wave, "gx", 0, 0, tiled=True)
    comp, table = transform(spectra, kernel_mesh)
    sent, order = splines(kernel_mesh, comp, table, wave)
    got = lax.all_to_all(sent, "gx", 0, 0, tiled=True).reshape(-1, LANES)

    push, weight = edges(order, density, wave_gradient)
    forward, backward = neighbours("gx")
    push = jnp.concatenate(
        [lax.ppermute(push[1:], "gx", forward), lax.ppermute(push[:1], "gx", backward)], axis=0
    )
    forward, backward = neighbours("yz")
    got = pltpu.with_memory_space_constraint(got, pltpu.VMEM)
    third = faces(got, weight, width)
    low = lax.ppermute(third[1], "yz", forward)
    high = lax.ppermute(third[0], "yz", backward)
    part = inner(got, push, density, wave_density, wave_gradient)
    return outer(part, low, high)


def solution(mesh):
    return jax.shard_map(
        shards,
        mesh=mesh,
        in_specs=(
            P(None, None, None, "gx", "yz"),
            P(),
            P("gx", None, "yz"),
            P("gx", None, "yz"),
            P("gx", None, "yz"),
            P(None, "gx", None, "yz"),
        ),
        out_specs=P("gx", None, "yz"),
        check_vma=False,
    )
```

```python
import functools
import math

import jax
import jax.numpy as jnp
import numpy as np
from jax import lax
from jax.experimental import pallas as pl
from jax.experimental.pallas import tpu as pltpu
from jax.sharding import PartitionSpec as P

LANES = 128
POINTS = 20
GROUP = 4
SLICES = 4
AHEAD = 8
BLOCKS_AHEAD = 4
IH, LOW, INV, ROWS = 0, 20, 40, 60


def in_hbm(array):
    return pltpu.with_memory_space_constraint(array, pltpu.HBM)


def half_tables(length):
    half = length // 2
    cells = np.arange(half)[:, None]
    tables = []
    for parity in range(2):
        waves = 2 * np.arange(half)[None, :] + parity
        angles = 2.0 * math.pi * (waves * cells % length) / length
        tables.append(np.concatenate([np.cos(angles), -np.sin(angles)], axis=1))
    return np.stack(tables).astype(jnp.bfloat16)


def spline_table(mesh_ref, table_ref):
    tile = (8, LANES)
    mesh = [jnp.full(tile, mesh_ref[j], jnp.float32) for j in range(POINTS)]
    steps = [mesh[j + 1] - mesh[j] for j in range(POINTS - 1)]
    for j in range(POINTS - 1):
        table_ref[IH + j] = 1.0 / steps[j]
    low = jnp.zeros(tile, jnp.float32)
    for j in range(1, POINTS - 1):
        pivot = (steps[j - 1] + steps[j]) / 3.0 - low * (steps[j - 1] / 6.0)
        inverse = 1.0 / pivot
        table_ref[LOW + j] = low
        table_ref[INV + j] = inverse
        low = (steps[j] / 6.0) * inverse
    table_ref[LOW + POINTS - 1] = low


def transform_kernel(mesh_ref, tables_hbm, spectra_ref, comp_ref, table_ref, tables_ref, held, wide, done, arrived, left):
    length = comp_ref.shape[1]
    half = length // 2
    groups = POINTS // GROUP

    def copy(c):
        return pltpu.make_async_copy(spectra_ref.at[:, c], held.at[c], arrived.at[c])

    def store(g, slot):
        return pltpu.make_async_copy(done.at[slot], comp_ref.at[pl.ds(g * (2 * GROUP), 2 * GROUP)], left.at[slot])

    tables_copy = pltpu.make_async_copy(tables_hbm, tables_ref, left.at[2])
    copy(0).start()
    tables_copy.start()
    for c in range(1, AHEAD):
        copy(c).start()
    spline_table(mesh_ref, table_ref)
    tables_copy.wait()

    def group(g, carry):
        slot = lax.rem(g, 2)

        @pl.when(g >= 2)
        def _():
            store(g - 2, slot).wait()

        for i in range(GROUP):
            c = g * GROUP + i
            copy(c).wait()

            @pl.when(c + AHEAD < POINTS)
            def _():
                copy(c + AHEAD).start()

        for i in range(GROUP):
            c = g * GROUP + i
            for p in range(2):
                wide[i, p] = held[c, p].astype(jnp.float32)
            parts = []
            for parity in range(2):
                operand = jnp.concatenate(
                    [
                        jnp.concatenate(
                            [
                                wide[i, p, pl.ds(2 * parity + y, half, stride=4), :].astype(jnp.bfloat16)
                                for y in range(2)
                            ],
                            axis=1,
                        )
                        for p in range(2)
                    ],
                    axis=0,
                )
                parts.append(jnp.dot(tables_ref[parity], operand, preferred_element_type=jnp.float32))
            total, difference = parts[0] + parts[1], parts[0] - parts[1]
            for y in range(2):
                done[slot, 2 * i + y, :half, :] = total[:, y * LANES : (y + 1) * LANES]
                done[slot, 2 * i + y, half:, :] = difference[:, y * LANES : (y + 1) * LANES]
        store(g, slot).start()
        return carry

    lax.fori_loop(0, groups, group, 0)
    for g in range(groups - 2, groups):
        store(g, g % 2).wait()


def transform(spectra, kernel_mesh):
    comps, length = spectra.shape[1], spectra.shape[2]
    tables = jnp.asarray(half_tables(length))
    flat = spectra.reshape(2, comps, 2 * length, LANES)
    return pl.pallas_call(
        transform_kernel,
        in_specs=[
            pl.BlockSpec(memory_space=pltpu.SMEM),
            pl.BlockSpec(memory_space=pltpu.HBM),
            pl.BlockSpec(memory_space=pltpu.HBM),
        ],
        out_specs=[pl.BlockSpec(memory_space=pltpu.HBM), pl.BlockSpec(memory_space=pltpu.VMEM)],
        out_shape=[
            pltpu.HBM((2 * comps, length, LANES), jnp.float32),
            jax.ShapeDtypeStruct((ROWS, 8, LANES), jnp.float32),
        ],
        scratch_shapes=[
            pltpu.VMEM((2, length // 2, length), jnp.bfloat16),
            pltpu.VMEM((comps, 2, 2 * length, LANES), jnp.bfloat16),
            pltpu.VMEM((GROUP, 2, 2 * length, LANES), jnp.float32),
            pltpu.VMEM((2, 2 * GROUP, length, LANES), jnp.float32),
            pltpu.SemaphoreType.DMA((comps,)),
            pltpu.SemaphoreType.DMA((3,)),
        ],
        compiler_params=pltpu.CompilerParams(vmem_limit_bytes=40 * 1024 * 1024),
        cost_estimate=pl.CostEstimate(
            flops=4 * comps * length * length * LANES,
            bytes_accessed=12 * comps * length * 2 * LANES,
            transcendentals=0,
        ),
        name="transform",
    )(kernel_mesh, in_hbm(tables), in_hbm(flat))


def solve(comp, table):
    before = (comp(1) - comp(0)) * table(IH)
    forward = [None] * POINTS
    for j in range(1, POINTS - 1):
        step = (comp(j + 1) - comp(j)) * table(IH + j)
        forward[j] = step - before
        if j > 1:
            forward[j] = forward[j] - table(LOW + j) * forward[j - 1]
        before = step
    second = [None] * POINTS
    for j in range(POINTS - 2, 0, -1):
        second[j] = forward[j] * table(INV + j)
        if j < POINTS - 2:
            second[j] = second[j] - table(LOW + j + 1) * second[j + 1]
    second[0] = second[POINTS - 1] = jnp.zeros_like(before)
    return second


def evaluate(comp, second, mesh, wave):
    def pick(node):
        held = [node(POINTS - 4 + i) for i in range(4)]
        for first in range(POINTS - 7, 0, -3):
            below = wave < mesh(first + 3)
            held = [jnp.where(below, node(first + i), held[i]) for i in range(4)]
        below = wave < mesh(1)
        return [jnp.where(below, node(min(i, 1)), held[i]) for i in range(4)]

    def ends(four, past_one, past_two):
        lower = jnp.where(past_two, four[2], jnp.where(past_one, four[1], four[0]))
        upper = jnp.where(past_two, four[3], jnp.where(past_one, four[2], four[1]))
        return lower, upper

    points_four = pick(mesh)
    past_one, past_two = wave >= points_four[1], wave >= points_four[2]
    low, high = ends(points_four, past_one, past_two)
    comp_low, comp_high = ends(pick(comp), past_one, past_two)
    second_low, second_high = ends(pick(second), past_one, past_two)
    width = high - low
    inverse = 1.0 / width
    a = (high - wave) * inverse
    b = (wave - low) * inverse
    sixth = width * (1.0 / 6.0)
    a2, b2 = a * a, b * b
    value = a * comp_low + b * comp_high + (
        (a2 - 1.0) * a * second_low + (b2 - 1.0) * b * second_high
    ) * (width * sixth)
    slope = (comp_high - comp_low) * inverse + (
        (3.0 * b2 - 1.0) * second_high - (3.0 * a2 - 1.0) * second_low
    ) * sixth
    return value, slope


def spline_kernel(scale, mesh_ref, table_ref, wave_ref, comp_ref, out_hbm, order_ref, out_ref, held, arrived, left):
    count, width = wave_ref.shape[0], wave_ref.shape[2]
    tiles = width // 8
    part = 2 * width + 4

    def copy(block):
        rows = pl.ds(pl.multiple_of(block * width, 8), width)
        return pltpu.make_async_copy(comp_ref.at[:, rows], held.at[block], arrived.at[block])

    def store(block):
        return pltpu.make_async_copy(out_ref.at[block], out_hbm.at[block], left.at[block])

    for block in range(BLOCKS_AHEAD):
        copy(block).start()
    order_ref[...] = jnp.zeros_like(order_ref)
    out_ref[count - 1] = jnp.zeros(out_ref.shape[1:], jnp.float32)
    mesh = [jnp.full((8, LANES), mesh_ref[j], jnp.float32) for j in range(POINTS)]

    def turn(block):
        slopes = [out_ref[block, y * part + width : y * part + 2 * width, :] for y in range(2)]
        slopes.append(jnp.zeros((LANES - 2 * width, LANES), jnp.float32))
        turned = jnp.concatenate(slopes, axis=0).T
        for side, edge in enumerate((turned[:1], turned[LANES - 1 :])):
            at = 2 * width + 2 + side
            out_ref[block, at : at + 1, :] = edge
            out_ref[block, part + at : part + at + 1, :] = pltpu.roll(edge, LANES - width, 1)

    def body(block, carry):
        following = lax.rem(block + 1, count)
        previous = lax.rem(block + count - 1, count)
        copy(block).wait()

        @pl.when(block + BLOCKS_AHEAD < count)
        def _():
            copy(block + BLOCKS_AHEAD).start()

        turn(previous)
        for y in range(2):
            wave = wave_ref[block, y].reshape(tiles, 8, LANES)
            comp = lambda j: held[block, 2 * j + y].reshape(tiles, 8, LANES)
            second = solve(comp, lambda j: table_ref[j])
            value, slope = evaluate(comp, lambda j: second[j], lambda j: mesh[j], wave)
            value = (value * scale).reshape(width, LANES)
            slope = (slope * scale).reshape(width, LANES)
            out_ref[block, y * part : y * part + width, :] = value
            out_ref[block, y * part + width : y * part + 2 * width, :] = slope
            at = y * part + 2 * width
            out_ref[following, at : at + 1, :] = slope[width - 1 :]
            out_ref[previous, at + 1 : at + 2, :] = slope[:1]
        @pl.when(block >= 2)
        def _():
            store(block - 1).start()

        return carry

    lax.fori_loop(0, count, body, 0)
    turn(count - 1)
    store(0).start()
    store(count - 1).start()
    for block in range(count):
        store(block).wait()


def splines(kernel_mesh, comp, table, wave):
    count, width = wave.shape[0], wave.shape[2]
    planes, length = comp.shape[0], comp.shape[1]
    vmem = pl.BlockSpec(memory_space=pltpu.VMEM)
    hbm = pl.BlockSpec(memory_space=pltpu.HBM)
    message = (count, 4 * width + 8, LANES)
    return pl.pallas_call(
        functools.partial(spline_kernel, length ** (-0.5)),
        in_specs=[pl.BlockSpec(memory_space=pltpu.SMEM), vmem, vmem, hbm],
        out_specs=[hbm, vmem],
        out_shape=[pltpu.HBM(message, jnp.float32), jax.ShapeDtypeStruct((8, LANES), jnp.float32)],
        scratch_shapes=[
            pltpu.VMEM(message, jnp.float32),
            pltpu.VMEM((count, planes, width, LANES), jnp.float32),
            pltpu.SemaphoreType.DMA((count,)),
            pltpu.SemaphoreType.DMA((count,)),
        ],
        compiler_params=pltpu.CompilerParams(vmem_limit_bytes=28 * 1024 * 1024),
        name="splines",
    )(kernel_mesh, table, wave, in_hbm(comp))


def edges_kernel(order_ref, density_ref, gradient_ref, push_ref, weight_ref, density, first, third, arrived):
    width, rows = density_ref.shape[0], density_ref.shape[1]
    copies = [
        pltpu.make_async_copy(density_ref, density, arrived.at[0]),
        pltpu.make_async_copy(gradient_ref.at[2], third, arrived.at[1]),
        pltpu.make_async_copy(gradient_ref.at[0, 0], first.at[0], arrived.at[2]),
        pltpu.make_async_copy(gradient_ref.at[0, width - 1], first.at[1], arrived.at[3]),
    ]
    for copy in copies:
        copy.start()
    for copy in copies:
        copy.wait()
    push_ref[0] = density[0] * first[0]
    push_ref[1] = density[width - 1] * first[1]
    lane = lax.broadcasted_iota(jnp.int32, (rows, LANES), 1)
    low = order_ref[:1] + jnp.zeros((rows, LANES), jnp.float32)
    high = low
    for x in range(width):
        product = density[x] * third[x]
        low = jnp.where(lane == x, product[:, :1], low)
        high = jnp.where(lane == x, product[:, LANES - 1 :], high)
    weight_ref[0] = low
    weight_ref[1] = high


def edges(order, density, gradient):
    rows = density.shape[1]
    vmem, hbm = pl.BlockSpec(memory_space=pltpu.VMEM), pl.BlockSpec(memory_space=pltpu.HBM)
    face = jax.ShapeDtypeStruct((2, rows, LANES), jnp.float32)
    return pl.pallas_call(
        edges_kernel,
        in_specs=[vmem, hbm, hbm],
        out_specs=[vmem, vmem],
        out_shape=[face, face],
        scratch_shapes=[
            pltpu.VMEM(density.shape, jnp.float32),
            pltpu.VMEM((2, rows, LANES), jnp.float32),
            pltpu.VMEM(density.shape, jnp.float32),
            pltpu.SemaphoreType.DMA((4,)),
        ],
        compiler_params=pltpu.CompilerParams(vmem_limit_bytes=8 * 1024 * 1024),
        name="edges",
    )(order, in_hbm(density), in_hbm(gradient))


def faces_kernel(width, got_ref, weight_ref, low_ref, high_ref):
    part, rows = 2 * width + 4, weight_ref.shape[1]
    for side, out_ref in enumerate((low_ref, high_ref)):
        out_ref[...] = got_ref[pl.ds(2 * width + 2 + side, rows, stride=part), :] * weight_ref[side]


def faces(got, weight, width):
    vmem = pl.BlockSpec(memory_space=pltpu.VMEM)
    return pl.pallas_call(
        functools.partial(faces_kernel, width),
        in_specs=[vmem, vmem],
        out_specs=[vmem, vmem],
        out_shape=[jax.ShapeDtypeStruct(weight.shape[1:], jnp.float32)] * 2,
        compiler_params=pltpu.CompilerParams(vmem_limit_bytes=8 * 1024 * 1024),
        name="faces",
    )(got, weight)


def inner_kernel(got_ref, push_ref, density_ref, rate_ref, gradient_ref, result, density, rate, gradient, arrived):
    width, rows = density_ref.shape[0], density_ref.shape[1]
    part = 2 * width + 4
    share = width // SLICES

    def copies(n):
        at = pl.ds(n * share, share)
        return [
            pltpu.make_async_copy(density_ref.at[at], density.at[at], arrived.at[n, 0]),
            pltpu.make_async_copy(rate_ref.at[at], rate.at[at], arrived.at[n, 1]),
            pltpu.make_async_copy(gradient_ref.at[:, at], gradient.at[:, at], arrived.at[n, 2]),
        ]

    for n in range(SLICES):
        for copy in copies(n):
            copy.start()

    def field(at):
        return got_ref[pl.ds(at, rows, stride=part), :]

    lane = lax.broadcasted_iota(jnp.int32, (rows, LANES), 1)
    ready = 0
    slope = [None] * width
    first = [None] * width
    for x in range(-1, width):
        ahead = x + 1
        if ahead < width:
            if ahead % share == 0:
                for copy in copies(ahead // share):
                    copy.wait()
            slope[ahead] = field(width + ahead) * density[ahead]
            first[ahead] = slope[ahead] * gradient[0, ahead]
        if x < 0:
            continue
        below = first[x - 1] if x > 0 else field(2 * width) * push_ref[0]
        above = first[x + 1] if x + 1 < width else field(2 * width + 1) * push_ref[1]
        second = slope[x] * gradient[1, x]
        third = slope[x] * gradient[2, x]
        beyond = jnp.where(lane == LANES - 1, 0.0, pltpu.roll(third, LANES - 1, 1))
        behind = jnp.where(lane == 0, 0.0, pltpu.roll(third, 1, 1))
        divergence = (above - below) + (beyond - behind)
        divergence = divergence + (pltpu.roll(second, rows - 1, 0) - pltpu.roll(second, 1, 0))
        result[x] = field(x) + rate[x] * slope[x] - 0.5 * divergence


def inner(got, push, density, rate, gradient):
    vmem, hbm = pl.BlockSpec(memory_space=pltpu.VMEM), pl.BlockSpec(memory_space=pltpu.HBM)
    return pl.pallas_call(
        inner_kernel,
        in_specs=[vmem, vmem, hbm, hbm, hbm],
        out_specs=vmem,
        out_shape=jax.ShapeDtypeStruct(density.shape, jnp.float32),
        scratch_shapes=[
            pltpu.VMEM(density.shape, jnp.float32),
            pltpu.VMEM(density.shape, jnp.float32),
            pltpu.VMEM(gradient.shape, jnp.float32),
            pltpu.SemaphoreType.DMA((SLICES, 3)),
        ],
        compiler_params=pltpu.CompilerParams(vmem_limit_bytes=16 * 1024 * 1024),
        name="inner",
    )(got, push, in_hbm(density), in_hbm(rate), in_hbm(gradient))


def outer_kernel(part_ref, low_ref, high_ref, out_hbm, out_ref, left):
    width, rows = part_ref.shape[0], part_ref.shape[1]
    share = width // SLICES
    lane = lax.broadcasted_iota(jnp.int32, (rows, LANES), 1)

    def store(n):
        at = pl.ds(n * share, share)
        return pltpu.make_async_copy(out_ref.at[at], out_hbm.at[at], left.at[n])

    for x in range(width):
        high = jnp.where(lane == LANES - 1, high_ref[:, x : x + 1], 0.0)
        flux = jnp.where(lane == 0, low_ref[:, x : x + 1], 0.0) - high
        out_ref[x] = part_ref[x] + 0.5 * flux
        if (x + 1) % share == 0:
            store(x // share).start()
    for n in range(SLICES):
        store(n).wait()


def outer(part, low, high):
    vmem, hbm = pl.BlockSpec(memory_space=pltpu.VMEM), pl.BlockSpec(memory_space=pltpu.HBM)
    return pl.pallas_call(
        outer_kernel,
        in_specs=[vmem] * 3,
        out_specs=hbm,
        out_shape=jax.ShapeDtypeStruct(part.shape, jnp.float32),
        scratch_shapes=[pltpu.VMEM(part.shape, jnp.float32), pltpu.SemaphoreType.DMA((SLICES,))],
        compiler_params=pltpu.CompilerParams(vmem_limit_bytes=8 * 1024 * 1024),
        name="outer",
    )(part, low, high)


def neighbours(axis):
    count = lax.axis_size(axis)
    forward = [(i, (i + 1) % count) for i in range(count)]
    return forward, [(target, source) for source, target in forward]


def turn_kernel(wave_ref, out_ref, held, arrived):
    width, rows = wave_ref.shape[0], wave_ref.shape[1]
    share = width // SLICES

    def copy(n):
        at = pl.ds(n * share, share)
        return pltpu.make_async_copy(wave_ref.at[at], held.at[at], arrived.at[n])

    for n in range(SLICES):
        copy(n).start()
    for x in range(width):
        if x % share == 0:
            copy(x // share).wait()
        out_ref[pl.ds(x, rows, stride=width), :] = held[x]


def turn(wave):
    width, rows = wave.shape[0], wave.shape[1]
    return pl.pallas_call(
        turn_kernel,
        in_specs=[pl.BlockSpec(memory_space=pltpu.HBM)],
        out_specs=pl.BlockSpec(memory_space=pltpu.VMEM),
        out_shape=jax.ShapeDtypeStruct((rows * width, LANES), jnp.float32),
        scratch_shapes=[pltpu.VMEM(wave.shape, jnp.float32), pltpu.SemaphoreType.DMA((SLICES,))],
        compiler_params=pltpu.CompilerParams(vmem_limit_bytes=8 * 1024 * 1024),
        name="turn",
    )(in_hbm(wave))


def shards(spectra, kernel_mesh, density, local_wave, wave_density, wave_gradient):
    width, rows = density.shape[0], density.shape[1]
    count = lax.axis_size("gx")
    wave = turn(local_wave).reshape(count, 2, width, LANES)
    wave = lax.all_to_all(wave, "gx", 0, 0, tiled=True)
    comp, table = transform(spectra, kernel_mesh)
    sent, order = splines(kernel_mesh, comp, table, wave)
    got = lax.all_to_all(sent, "gx", 0, 0, tiled=True).reshape(-1, LANES)

    push, weight = edges(order, density, wave_gradient)
    forward, backward = neighbours("gx")
    push = jnp.concatenate(
        [lax.ppermute(push[1:], "gx", forward), lax.ppermute(push[:1], "gx", backward)], axis=0
    )
    forward, backward = neighbours("yz")
    got = pltpu.with_memory_space_constraint(got, pltpu.VMEM)
    third_low, third_high = faces(got, weight, width)
    low = lax.ppermute(third_high, "yz", forward)
    high = lax.ppermute(third_low, "yz", backward)
    part = inner(got, push, density, wave_density, wave_gradient)
    return outer(part, low, high)


def solution(mesh):
    return jax.shard_map(
        shards,
        mesh=mesh,
        in_specs=(
            P(None, None, None, "gx", "yz"),
            P(),
            P("gx", None, "yz"),
            P("gx", None, "yz"),
            P("gx", None, "yz"),
            P(None, "gx", None, "yz"),
        ),
        out_specs=P("gx", None, "yz"),
        check_vma=False,
    )
```

```python
import functools
import math

import jax
import jax.numpy as jnp
import numpy as np
from jax import lax
from jax.experimental import pallas as pl
from jax.experimental.pallas import tpu as pltpu
from jax.sharding import PartitionSpec as P

LANES = 128
POINTS = 20
GROUPS = (2, 4, 6, 5, 3)
SLICES = 4
AHEAD = 10
BLOCKS_AHEAD = 4
IH, LOW, INV, ROWS = 0, 20, 40, 60


def in_hbm(array):
    return pltpu.with_memory_space_constraint(array, pltpu.HBM)


def half_tables(length):
    half = length // 2
    cells = np.arange(half)[:, None]
    tables = []
    for parity in range(2):
        waves = 2 * np.arange(half)[None, :] + parity
        angles = 2.0 * math.pi * (waves * cells % length) / length
        tables.append(np.concatenate([np.cos(angles), -np.sin(angles)], axis=1))
    return np.stack(tables).astype(jnp.bfloat16)


def spline_table(mesh_ref, table_ref):
    tile = (8, LANES)
    mesh = [jnp.full(tile, mesh_ref[j], jnp.float32) for j in range(POINTS)]
    steps = [mesh[j + 1] - mesh[j] for j in range(POINTS - 1)]
    for j in range(POINTS - 1):
        table_ref[IH + j] = 1.0 / steps[j]
    low = jnp.zeros(tile, jnp.float32)
    for j in range(1, POINTS - 1):
        pivot = (steps[j - 1] + steps[j]) / 3.0 - low * (steps[j - 1] / 6.0)
        inverse = 1.0 / pivot
        table_ref[LOW + j] = low
        table_ref[INV + j] = inverse
        low = (steps[j] / 6.0) * inverse
    table_ref[LOW + POINTS - 1] = low


def transform_kernel(mesh_ref, tables_hbm, spectra_ref, comp_ref, table_ref, tables_ref, held, wide, done, arrived, left):
    length = comp_ref.shape[1]
    half = length // 2

    def copy(c):
        return pltpu.make_async_copy(spectra_ref.at[:, c], held.at[c], arrived.at[c])

    def store(start, size, slot):
        planes = pl.ds(2 * start, 2 * size)
        return pltpu.make_async_copy(done.at[slot, pl.ds(0, 2 * size)], comp_ref.at[planes], left.at[slot])

    tables_copy = pltpu.make_async_copy(tables_hbm, tables_ref, left.at[2])
    copy(0).start()
    tables_copy.start()
    for c in range(1, AHEAD):
        copy(c).start()
    spline_table(mesh_ref, table_ref)
    tables_copy.wait()

    starts = [sum(GROUPS[:g]) for g in range(len(GROUPS))]
    for g, (start, size) in enumerate(zip(starts, GROUPS)):
        slot = g % 2
        if g >= 2:
            store(starts[g - 2], GROUPS[g - 2], slot).wait()
        for c in range(start, start + size):
            copy(c).wait()
            if c + AHEAD < POINTS:
                copy(c + AHEAD).start()
        for i in range(size):
            c = start + i
            for p in range(2):
                wide[i, p] = held[c, p].astype(jnp.float32)
            parts = []
            for parity in range(2):
                operand = jnp.concatenate(
                    [
                        jnp.concatenate(
                            [
                                wide[i, p, pl.ds(2 * parity + y, half, stride=4), :].astype(jnp.bfloat16)
                                for y in range(2)
                            ],
                            axis=1,
                        )
                        for p in range(2)
                    ],
                    axis=0,
                )
                parts.append(jnp.dot(tables_ref[parity], operand, preferred_element_type=jnp.float32))
            total, difference = parts[0] + parts[1], parts[0] - parts[1]
            for y in range(2):
                done[slot, 2 * i + y, :half, :] = total[:, y * LANES : (y + 1) * LANES]
                done[slot, 2 * i + y, half:, :] = difference[:, y * LANES : (y + 1) * LANES]
        store(start, size, slot).start()
    for g in range(len(GROUPS) - 2, len(GROUPS)):
        store(starts[g], GROUPS[g], g % 2).wait()


def transform(spectra, kernel_mesh):
    comps, length = spectra.shape[1], spectra.shape[2]
    tables = jnp.asarray(half_tables(length))
    flat = spectra.reshape(2, comps, 2 * length, LANES)
    return pl.pallas_call(
        transform_kernel,
        in_specs=[
            pl.BlockSpec(memory_space=pltpu.SMEM),
            pl.BlockSpec(memory_space=pltpu.HBM),
            pl.BlockSpec(memory_space=pltpu.HBM),
        ],
        out_specs=[pl.BlockSpec(memory_space=pltpu.HBM), pl.BlockSpec(memory_space=pltpu.VMEM)],
        out_shape=[
            pltpu.HBM((2 * comps, length, LANES), jnp.float32),
            jax.ShapeDtypeStruct((ROWS, 8, LANES), jnp.float32),
        ],
        scratch_shapes=[
            pltpu.VMEM((2, length // 2, length), jnp.bfloat16),
            pltpu.VMEM((comps, 2, 2 * length, LANES), jnp.bfloat16),
            pltpu.VMEM((max(GROUPS), 2, 2 * length, LANES), jnp.float32),
            pltpu.VMEM((2, 2 * max(GROUPS), length, LANES), jnp.float32),
            pltpu.SemaphoreType.DMA((comps,)),
            pltpu.SemaphoreType.DMA((3,)),
        ],
        compiler_params=pltpu.CompilerParams(vmem_limit_bytes=40 * 1024 * 1024),
        cost_estimate=pl.CostEstimate(
            flops=4 * comps * length * length * LANES,
            bytes_accessed=12 * comps * length * 2 * LANES,
            transcendentals=0,
        ),
        name="transform",
    )(kernel_mesh, in_hbm(tables), in_hbm(flat))


def solve(comp, table):
    before = (comp(1) - comp(0)) * table(IH)
    forward = [None] * POINTS
    for j in range(1, POINTS - 1):
        step = (comp(j + 1) - comp(j)) * table(IH + j)
        forward[j] = step - before
        if j > 1:
            forward[j] = forward[j] - table(LOW + j) * forward[j - 1]
        before = step
    second = [None] * POINTS
    for j in range(POINTS - 2, 0, -1):
        second[j] = forward[j] * table(INV + j)
        if j < POINTS - 2:
            second[j] = second[j] - table(LOW + j + 1) * second[j + 1]
    second[0] = second[POINTS - 1] = jnp.zeros_like(before)
    return second


def evaluate(comp, second, mesh, wave):
    top = wave >= mesh(16)

    def halve(nodes, past):
        half = len(nodes) // 2
        return [jnp.where(past, nodes[half + k], nodes[k]) for k in range(half + 1)]

    def spread(node):
        nodes = [node(k) for k in range(17)]
        return [jnp.where(top, node(16 + k), nodes[k]) for k in range(4)] + nodes[4:]

    nodes, turns = spread(mesh), []
    for half in (8, 4, 2, 1):
        past = wave >= nodes[half]
        if half >= 4:
            past = past & ~top
        if half == 1:
            past = past & (wave < mesh(POINTS - 2))
        turns.append(past)
        nodes = halve(nodes, past)
    low, high = nodes

    def pick(node):
        nodes = spread(node)
        for past in turns:
            nodes = halve(nodes, past)
        return nodes

    comp_low, comp_high = pick(comp)
    second_low, second_high = pick(second)
    width = high - low
    inverse = 1.0 / width
    a = (high - wave) * inverse
    b = (wave - low) * inverse
    sixth = width * (1.0 / 6.0)
    a2, b2 = a * a, b * b
    value = a * comp_low + b * comp_high + (
        (a2 - 1.0) * a * second_low + (b2 - 1.0) * b * second_high
    ) * (width * sixth)
    slope = (comp_high - comp_low) * inverse + (
        (3.0 * b2 - 1.0) * second_high - (3.0 * a2 - 1.0) * second_low
    ) * sixth
    return value, slope


def spline_kernel(scale, mesh_ref, table_ref, wave_ref, comp_ref, out_hbm, order_ref, out_ref, held, arrived, left):
    count, width = wave_ref.shape[0], wave_ref.shape[2]
    tiles = width // 8
    part = 2 * width + 4

    def copy(block):
        rows = pl.ds(pl.multiple_of(block * width, 8), width)
        return pltpu.make_async_copy(comp_ref.at[:, rows], held.at[block], arrived.at[block])

    def store(block):
        return pltpu.make_async_copy(out_ref.at[block], out_hbm.at[block], left.at[block])

    for block in range(BLOCKS_AHEAD):
        copy(block).start()
    order_ref[...] = jnp.zeros_like(order_ref)
    out_ref[count - 1] = jnp.zeros(out_ref.shape[1:], jnp.float32)
    mesh = [jnp.full((8, LANES), mesh_ref[j], jnp.float32) for j in range(POINTS)]

    def turn(block):
        slopes = [out_ref[block, y * part + width : y * part + 2 * width, :] for y in range(2)]
        slopes.append(jnp.zeros((LANES - 2 * width, LANES), jnp.float32))
        turned = jnp.concatenate(slopes, axis=0).T
        for side, edge in enumerate((turned[:1], turned[LANES - 1 :])):
            at = 2 * width + 2 + side
            out_ref[block, at : at + 1, :] = edge
            out_ref[block, part + at : part + at + 1, :] = pltpu.roll(edge, LANES - width, 1)

    def body(block, carry):
        following = lax.rem(block + 1, count)
        previous = lax.rem(block + count - 1, count)
        copy(block).wait()

        @pl.when(block + BLOCKS_AHEAD < count)
        def _():
            copy(block + BLOCKS_AHEAD).start()

        turn(previous)
        for y in range(2):
            wave = wave_ref[block, y].reshape(tiles, 8, LANES)
            comp = lambda j: held[block, 2 * j + y].reshape(tiles, 8, LANES)
            second = solve(comp, lambda j: table_ref[j])
            value, slope = evaluate(comp, lambda j: second[j], lambda j: mesh[j], wave)
            value = (value * scale).reshape(width, LANES)
            slope = (slope * scale).reshape(width, LANES)
            out_ref[block, y * part : y * part + width, :] = value
            out_ref[block, y * part + width : y * part + 2 * width, :] = slope
            at = y * part + 2 * width
            out_ref[following, at : at + 1, :] = slope[width - 1 :]
            out_ref[previous, at + 1 : at + 2, :] = slope[:1]
        @pl.when(block >= 2)
        def _():
            store(block - 1).start()

        return carry

    lax.fori_loop(0, count, body, 0)
    turn(count - 1)
    store(0).start()
    store(count - 1).start()
    for block in range(count):
        store(block).wait()


def splines(kernel_mesh, comp, table, wave):
    count, width = wave.shape[0], wave.shape[2]
    planes, length = comp.shape[0], comp.shape[1]
    vmem = pl.BlockSpec(memory_space=pltpu.VMEM)
    hbm = pl.BlockSpec(memory_space=pltpu.HBM)
    message = (count, 4 * width + 8, LANES)
    return pl.pallas_call(
        functools.partial(spline_kernel, length ** (-0.5)),
        in_specs=[pl.BlockSpec(memory_space=pltpu.SMEM), vmem, vmem, hbm],
        out_specs=[hbm, vmem],
        out_shape=[pltpu.HBM(message, jnp.float32), jax.ShapeDtypeStruct((8, LANES), jnp.float32)],
        scratch_shapes=[
            pltpu.VMEM(message, jnp.float32),
            pltpu.VMEM((count, planes, width, LANES), jnp.float32),
            pltpu.SemaphoreType.DMA((count,)),
            pltpu.SemaphoreType.DMA((count,)),
        ],
        compiler_params=pltpu.CompilerParams(vmem_limit_bytes=28 * 1024 * 1024),
        name="splines",
    )(kernel_mesh, table, wave, in_hbm(comp))


def edges_kernel(order_ref, density_ref, gradient_ref, push_ref, weight_ref, density, first, third, arrived):
    width, rows = density_ref.shape[0], density_ref.shape[1]
    copies = [
        pltpu.make_async_copy(density_ref, density, arrived.at[0]),
        pltpu.make_async_copy(gradient_ref.at[2], third, arrived.at[1]),
        pltpu.make_async_copy(gradient_ref.at[0, 0], first.at[0], arrived.at[2]),
        pltpu.make_async_copy(gradient_ref.at[0, width - 1], first.at[1], arrived.at[3]),
    ]
    for copy in copies:
        copy.start()
    for copy in copies:
        copy.wait()
    push_ref[0] = density[0] * first[0]
    push_ref[1] = density[width - 1] * first[1]
    lane = lax.broadcasted_iota(jnp.int32, (rows, LANES), 1)
    low = order_ref[:1] + jnp.zeros((rows, LANES), jnp.float32)
    high = low
    for x in range(width):
        product = density[x] * third[x]
        low = jnp.where(lane == x, product[:, :1], low)
        high = jnp.where(lane == x, product[:, LANES - 1 :], high)
    weight_ref[0] = low
    weight_ref[1] = high


def edges(order, density, gradient):
    rows = density.shape[1]
    vmem, hbm = pl.BlockSpec(memory_space=pltpu.VMEM), pl.BlockSpec(memory_space=pltpu.HBM)
    face = jax.ShapeDtypeStruct((2, rows, LANES), jnp.float32)
    return pl.pallas_call(
        edges_kernel,
        in_specs=[vmem, hbm, hbm],
        out_specs=[vmem, vmem],
        out_shape=[face, face],
        scratch_shapes=[
            pltpu.VMEM(density.shape, jnp.float32),
            pltpu.VMEM((2, rows, LANES), jnp.float32),
            pltpu.VMEM(density.shape, jnp.float32),
            pltpu.SemaphoreType.DMA((4,)),
        ],
        compiler_params=pltpu.CompilerParams(vmem_limit_bytes=8 * 1024 * 1024),
        name="edges",
    )(order, in_hbm(density), in_hbm(gradient))


def faces_kernel(width, got_ref, weight_ref, low_ref, high_ref):
    part, rows = 2 * width + 4, weight_ref.shape[1]
    for side, out_ref in enumerate((low_ref, high_ref)):
        out_ref[...] = got_ref[pl.ds(2 * width + 2 + side, rows, stride=part), :] * weight_ref[side]


def faces(got, weight, width):
    vmem = pl.BlockSpec(memory_space=pltpu.VMEM)
    return pl.pallas_call(
        functools.partial(faces_kernel, width),
        in_specs=[vmem, vmem],
        out_specs=[vmem, vmem],
        out_shape=[jax.ShapeDtypeStruct(weight.shape[1:], jnp.float32)] * 2,
        compiler_params=pltpu.CompilerParams(vmem_limit_bytes=8 * 1024 * 1024),
        name="faces",
    )(got, weight)


def inner_kernel(got_ref, push_ref, density_ref, rate_ref, gradient_ref, result, density, rate, gradient, arrived):
    width, rows = density_ref.shape[0], density_ref.shape[1]
    part = 2 * width + 4
    share = width // SLICES

    def copies(n):
        at = pl.ds(n * share, share)
        return [
            pltpu.make_async_copy(density_ref.at[at], density.at[at], arrived.at[n, 0]),
            pltpu.make_async_copy(rate_ref.at[at], rate.at[at], arrived.at[n, 1]),
            pltpu.make_async_copy(gradient_ref.at[:, at], gradient.at[:, at], arrived.at[n, 2]),
        ]

    for n in range(SLICES):
        for copy in copies(n):
            copy.start()

    def field(at):
        return got_ref[pl.ds(at, rows, stride=part), :]

    lane = lax.broadcasted_iota(jnp.int32, (rows, LANES), 1)
    ready = 0
    slope = [None] * width
    first = [None] * width
    for x in range(-1, width):
        ahead = x + 1
        if ahead < width:
            if ahead % share == 0:
                for copy in copies(ahead // share):
                    copy.wait()
            slope[ahead] = field(width + ahead) * density[ahead]
            first[ahead] = slope[ahead] * gradient[0, ahead]
        if x < 0:
            continue
        below = first[x - 1] if x > 0 else field(2 * width) * push_ref[0]
        above = first[x + 1] if x + 1 < width else field(2 * width + 1) * push_ref[1]
        second = slope[x] * gradient[1, x]
        third = slope[x] * gradient[2, x]
        beyond = jnp.where(lane == LANES - 1, 0.0, pltpu.roll(third, LANES - 1, 1))
        behind = jnp.where(lane == 0, 0.0, pltpu.roll(third, 1, 1))
        divergence = (above - below) + (beyond - behind)
        divergence = divergence + (pltpu.roll(second, rows - 1, 0) - pltpu.roll(second, 1, 0))
        result[x] = field(x) + rate[x] * slope[x] - 0.5 * divergence


def inner(got, push, density, rate, gradient):
    vmem, hbm = pl.BlockSpec(memory_space=pltpu.VMEM), pl.BlockSpec(memory_space=pltpu.HBM)
    return pl.pallas_call(
        inner_kernel,
        in_specs=[vmem, vmem, hbm, hbm, hbm],
        out_specs=vmem,
        out_shape=jax.ShapeDtypeStruct(density.shape, jnp.float32),
        scratch_shapes=[
            pltpu.VMEM(density.shape, jnp.float32),
            pltpu.VMEM(density.shape, jnp.float32),
            pltpu.VMEM(gradient.shape, jnp.float32),
            pltpu.SemaphoreType.DMA((SLICES, 3)),
        ],
        compiler_params=pltpu.CompilerParams(vmem_limit_bytes=16 * 1024 * 1024),
        name="inner",
    )(got, push, in_hbm(density), in_hbm(rate), in_hbm(gradient))


def outer_kernel(part_ref, low_ref, high_ref, out_hbm, out_ref, left):
    width, rows = part_ref.shape[0], part_ref.shape[1]
    share = width // SLICES
    lane = lax.broadcasted_iota(jnp.int32, (rows, LANES), 1)

    def store(n):
        at = pl.ds(n * share, share)
        return pltpu.make_async_copy(out_ref.at[at], out_hbm.at[at], left.at[n])

    for x in range(width):
        high = jnp.where(lane == LANES - 1, high_ref[:, x : x + 1], 0.0)
        flux = jnp.where(lane == 0, low_ref[:, x : x + 1], 0.0) - high
        out_ref[x] = part_ref[x] + 0.5 * flux
        if (x + 1) % share == 0:
            store(x // share).start()
    for n in range(SLICES):
        store(n).wait()


def outer(part, low, high):
    vmem, hbm = pl.BlockSpec(memory_space=pltpu.VMEM), pl.BlockSpec(memory_space=pltpu.HBM)
    return pl.pallas_call(
        outer_kernel,
        in_specs=[vmem] * 3,
        out_specs=hbm,
        out_shape=jax.ShapeDtypeStruct(part.shape, jnp.float32),
        scratch_shapes=[pltpu.VMEM(part.shape, jnp.float32), pltpu.SemaphoreType.DMA((SLICES,))],
        compiler_params=pltpu.CompilerParams(vmem_limit_bytes=8 * 1024 * 1024),
        name="outer",
    )(part, low, high)


def neighbours(axis):
    count = lax.axis_size(axis)
    forward = [(i, (i + 1) % count) for i in range(count)]
    return forward, [(target, source) for source, target in forward]


def turn_kernel(wave_ref, out_ref, held, arrived):
    width, rows = wave_ref.shape[0], wave_ref.shape[1]
    share = width // SLICES

    def copy(n):
        at = pl.ds(n * share, share)
        return pltpu.make_async_copy(wave_ref.at[at], held.at[at], arrived.at[n])

    for n in range(SLICES):
        copy(n).start()
    for x in range(width):
        if x % share == 0:
            copy(x // share).wait()
        out_ref[pl.ds(x, rows, stride=width), :] = held[x]


def turn(wave):
    width, rows = wave.shape[0], wave.shape[1]
    return pl.pallas_call(
        turn_kernel,
        in_specs=[pl.BlockSpec(memory_space=pltpu.HBM)],
        out_specs=pl.BlockSpec(memory_space=pltpu.VMEM),
        out_shape=pltpu.VMEM((rows * width, LANES), jnp.float32),
        scratch_shapes=[pltpu.VMEM(wave.shape, jnp.float32), pltpu.SemaphoreType.DMA((SLICES,))],
        compiler_params=pltpu.CompilerParams(vmem_limit_bytes=8 * 1024 * 1024),
        name="turn",
    )(in_hbm(wave))


def shards(spectra, kernel_mesh, density, local_wave, wave_density, wave_gradient):
    width, rows = density.shape[0], density.shape[1]
    count = lax.axis_size("gx")
    wave = turn(local_wave).reshape(count, 2, width, LANES)
    wave = lax.all_to_all(wave, "gx", 0, 0, tiled=True)
    comp, table = transform(spectra, kernel_mesh)
    sent, order = splines(kernel_mesh, comp, table, wave)
    got = lax.all_to_all(sent, "gx", 0, 0, tiled=True).reshape(-1, LANES)

    push, weight = edges(order, density, wave_gradient)
    forward, backward = neighbours("gx")
    push = jnp.concatenate(
        [lax.ppermute(push[1:], "gx", forward), lax.ppermute(push[:1], "gx", backward)], axis=0
    )
    forward, backward = neighbours("yz")
    got = pltpu.with_memory_space_constraint(got, pltpu.VMEM)
    third_low, third_high = faces(got, weight, width)
    low = lax.ppermute(third_high, "yz", forward)
    high = lax.ppermute(third_low, "yz", backward)
    part = inner(got, push, density, wave_density, wave_gradient)
    return outer(part, low, high)


def solution(mesh):
    return jax.shard_map(
        shards,
        mesh=mesh,
        in_specs=(
            P(None, None, None, "gx", "yz"),
            P(),
            P("gx", None, "yz"),
            P("gx", None, "yz"),
            P("gx", None, "yz"),
            P(None, "gx", None, "yz"),
        ),
        out_specs=P("gx", None, "yz"),
        check_vma=False,
    )
```

```python
import functools
import math

import jax
import jax.numpy as jnp
import numpy as np
from jax import lax
from jax.experimental import pallas as pl
from jax.experimental.pallas import tpu as pltpu
from jax.sharding import PartitionSpec as P

LANES = 128
POINTS = 20
KEPT = 4
GROUPS = (2, 4, 6, 4, 4)
SLICES = 4
AHEAD = 10
BLOCKS_AHEAD = 4
IH, LOW, INV, ROWS = 0, 20, 40, 60


def in_hbm(array):
    return pltpu.with_memory_space_constraint(array, pltpu.HBM)


def half_tables(length):
    half = length // 2
    cells = np.arange(half)[:, None]
    tables = []
    for parity in range(2):
        waves = 2 * np.arange(half)[None, :] + parity
        angles = 2.0 * math.pi * (waves * cells % length) / length
        tables.append(np.concatenate([np.cos(angles), -np.sin(angles)], axis=1))
    return np.stack(tables).astype(jnp.bfloat16)


def spline_table(mesh_ref, table_ref):
    tile = (8, LANES)
    mesh = [jnp.full(tile, mesh_ref[j], jnp.float32) for j in range(POINTS)]
    steps = [mesh[j + 1] - mesh[j] for j in range(POINTS - 1)]
    for j in range(POINTS - 1):
        table_ref[IH + j] = 1.0 / steps[j]
    low = jnp.zeros(tile, jnp.float32)
    for j in range(1, POINTS - 1):
        pivot = (steps[j - 1] + steps[j]) / 3.0 - low * (steps[j - 1] / 6.0)
        inverse = 1.0 / pivot
        table_ref[LOW + j] = low
        table_ref[INV + j] = inverse
        low = (steps[j] / 6.0) * inverse
    table_ref[LOW + POINTS - 1] = low


def transform_kernel(mesh_ref, tables_hbm, spectra_ref, comp_ref, kept_ref, table_ref, tables_ref, held, wide, done, arrived, left):
    length = comp_ref.shape[1]
    half = length // 2

    def copy(c):
        return pltpu.make_async_copy(spectra_ref.at[:, c], held.at[c], arrived.at[c])

    def store(start, size, slot):
        size = min(size, POINTS - KEPT - start)
        planes = pl.ds(2 * start, 2 * size)
        return pltpu.make_async_copy(done.at[slot, pl.ds(0, 2 * size)], comp_ref.at[planes], left.at[slot])

    tables_copy = pltpu.make_async_copy(tables_hbm, tables_ref, left.at[2])
    copy(0).start()
    tables_copy.start()
    for c in range(1, AHEAD):
        copy(c).start()
    spline_table(mesh_ref, table_ref)
    tables_copy.wait()

    starts = [sum(GROUPS[:g]) for g in range(len(GROUPS))]
    sent = [g for g in range(len(GROUPS)) if starts[g] < POINTS - KEPT]
    for g, (start, size) in enumerate(zip(starts, GROUPS)):
        slot = g % 2
        if g >= 2 and g in sent:
            store(starts[g - 2], GROUPS[g - 2], slot).wait()
        for c in range(start, start + size):
            copy(c).wait()
            if c + AHEAD < POINTS:
                copy(c + AHEAD).start()
        for i in range(size):
            c = start + i
            for p in range(2):
                wide[i, p] = held[c, p].astype(jnp.float32)
            parts = []
            for parity in range(2):
                operand = jnp.concatenate(
                    [
                        jnp.concatenate(
                            [
                                wide[i, p, pl.ds(2 * parity + y, half, stride=4), :].astype(jnp.bfloat16)
                                for y in range(2)
                            ],
                            axis=1,
                        )
                        for p in range(2)
                    ],
                    axis=0,
                )
                parts.append(jnp.dot(tables_ref[parity], operand, preferred_element_type=jnp.float32))
            total, difference = parts[0] + parts[1], parts[0] - parts[1]
            for y in range(2):
                if c < POINTS - KEPT:
                    plane = done.at[slot, 2 * i + y]
                else:
                    plane = kept_ref.at[2 * (c - POINTS + KEPT) + y]
                plane[:half, :] = total[:, y * LANES : (y + 1) * LANES]
                plane[half:, :] = difference[:, y * LANES : (y + 1) * LANES]
        if g in sent:
            store(start, size, slot).start()
    for g in sent[-2:]:
        store(starts[g], GROUPS[g], g % 2).wait()


def transform(spectra, kernel_mesh):
    comps, length = spectra.shape[1], spectra.shape[2]
    tables = jnp.asarray(half_tables(length))
    flat = spectra.reshape(2, comps, 2 * length, LANES)
    return pl.pallas_call(
        transform_kernel,
        in_specs=[
            pl.BlockSpec(memory_space=pltpu.SMEM),
            pl.BlockSpec(memory_space=pltpu.HBM),
            pl.BlockSpec(memory_space=pltpu.HBM),
        ],
        out_specs=[pl.BlockSpec(memory_space=pltpu.HBM)] + [pl.BlockSpec(memory_space=pltpu.VMEM)] * 2,
        out_shape=[
            pltpu.HBM((2 * (comps - KEPT), length, LANES), jnp.float32),
            jax.ShapeDtypeStruct((2 * KEPT, length, LANES), jnp.float32),
            jax.ShapeDtypeStruct((ROWS, 8, LANES), jnp.float32),
        ],
        scratch_shapes=[
            pltpu.VMEM((2, length // 2, length), jnp.bfloat16),
            pltpu.VMEM((comps, 2, 2 * length, LANES), jnp.bfloat16),
            pltpu.VMEM((max(GROUPS), 2, 2 * length, LANES), jnp.float32),
            pltpu.VMEM((2, 2 * max(GROUPS), length, LANES), jnp.float32),
            pltpu.SemaphoreType.DMA((comps,)),
            pltpu.SemaphoreType.DMA((3,)),
        ],
        compiler_params=pltpu.CompilerParams(vmem_limit_bytes=40 * 1024 * 1024),
        cost_estimate=pl.CostEstimate(
            flops=4 * comps * length * length * LANES,
            bytes_accessed=12 * comps * length * 2 * LANES,
            transcendentals=0,
        ),
        name="transform",
    )(kernel_mesh, in_hbm(tables), in_hbm(flat))


def solve(comp, table):
    before = (comp(1) - comp(0)) * table(IH)
    forward = [None] * POINTS
    for j in range(1, POINTS - 1):
        step = (comp(j + 1) - comp(j)) * table(IH + j)
        forward[j] = step - before
        if j > 1:
            forward[j] = forward[j] - table(LOW + j) * forward[j - 1]
        before = step
    second = [None] * POINTS
    for j in range(POINTS - 2, 0, -1):
        second[j] = forward[j] * table(INV + j)
        if j < POINTS - 2:
            second[j] = second[j] - table(LOW + j + 1) * second[j + 1]
    second[0] = second[POINTS - 1] = jnp.zeros_like(before)
    return second


def evaluate(comp, second, mesh, wave):
    top = wave >= mesh(16)

    def halve(nodes, past):
        half = len(nodes) // 2
        return [jnp.where(past, nodes[half + k], nodes[k]) for k in range(half + 1)]

    def spread(node):
        nodes = [node(k) for k in range(17)]
        return [jnp.where(top, node(16 + k), nodes[k]) for k in range(4)] + nodes[4:]

    nodes, turns = spread(mesh), []
    for half in (8, 4, 2, 1):
        past = wave >= nodes[half]
        if half >= 4:
            past = past & ~top
        if half == 1:
            past = past & (wave < mesh(POINTS - 2))
        turns.append(past)
        nodes = halve(nodes, past)
    low, high = nodes

    def pick(node):
        nodes = spread(node)
        for past in turns:
            nodes = halve(nodes, past)
        return nodes

    comp_low, comp_high = pick(comp)
    second_low, second_high = pick(second)
    width = high - low
    inverse = 1.0 / width
    a = (high - wave) * inverse
    b = (wave - low) * inverse
    sixth = width * (1.0 / 6.0)
    a2, b2 = a * a, b * b
    value = a * comp_low + b * comp_high + (
        (a2 - 1.0) * a * second_low + (b2 - 1.0) * b * second_high
    ) * (width * sixth)
    slope = (comp_high - comp_low) * inverse + (
        (3.0 * b2 - 1.0) * second_high - (3.0 * a2 - 1.0) * second_low
    ) * sixth
    return value, slope


def spline_kernel(scale, mesh_ref, table_ref, wave_ref, kept_ref, comp_ref, out_hbm, order_ref, out_ref, held, arrived, left):
    count, width = wave_ref.shape[0], wave_ref.shape[2]
    tiles = width // 8
    part = 2 * width + 4

    def copy(block):
        rows = pl.ds(pl.multiple_of(block * width, 8), width)
        return pltpu.make_async_copy(comp_ref.at[:, rows], held.at[block], arrived.at[block])

    def store(block):
        return pltpu.make_async_copy(out_ref.at[block], out_hbm.at[block], left.at[block])

    for block in range(BLOCKS_AHEAD):
        copy(block).start()
    order_ref[...] = jnp.zeros_like(order_ref)
    out_ref[count - 1] = jnp.zeros(out_ref.shape[1:], jnp.float32)
    mesh = [jnp.full((8, LANES), mesh_ref[j], jnp.float32) for j in range(POINTS)]

    def turn(block):
        slopes = [out_ref[block, y * part + width : y * part + 2 * width, :] for y in range(2)]
        slopes.append(jnp.zeros((LANES - 2 * width, LANES), jnp.float32))
        turned = jnp.concatenate(slopes, axis=0).T
        for side, edge in enumerate((turned[:1], turned[LANES - 1 :])):
            at = 2 * width + 2 + side
            out_ref[block, at : at + 1, :] = edge
            out_ref[block, part + at : part + at + 1, :] = pltpu.roll(edge, LANES - width, 1)

    def body(block, carry):
        following = lax.rem(block + 1, count)
        previous = lax.rem(block + count - 1, count)
        copy(block).wait()

        @pl.when(block + BLOCKS_AHEAD < count)
        def _():
            copy(block + BLOCKS_AHEAD).start()

        turn(previous)
        for y in range(2):
            wave = wave_ref[block, y].reshape(tiles, 8, LANES)

            def comp(j):
                if j < POINTS - KEPT:
                    return held[block, 2 * j + y].reshape(tiles, 8, LANES)
                rows = pl.ds(pl.multiple_of(block * width, 8), width)
                return kept_ref[2 * (j - POINTS + KEPT) + y, rows, :].reshape(tiles, 8, LANES)

            second = solve(comp, lambda j: table_ref[j])
            value, slope = evaluate(comp, lambda j: second[j], lambda j: mesh[j], wave)
            value = (value * scale).reshape(width, LANES)
            slope = (slope * scale).reshape(width, LANES)
            out_ref[block, y * part : y * part + width, :] = value
            out_ref[block, y * part + width : y * part + 2 * width, :] = slope
            at = y * part + 2 * width
            out_ref[following, at : at + 1, :] = slope[width - 1 :]
            out_ref[previous, at + 1 : at + 2, :] = slope[:1]
        @pl.when(block >= 2)
        def _():
            store(block - 1).start()

        return carry

    lax.fori_loop(0, count, body, 0)
    turn(count - 1)
    store(0).start()
    store(count - 1).start()
    for block in range(count):
        store(block).wait()


def splines(kernel_mesh, comp, kept, table, wave):
    count, width = wave.shape[0], wave.shape[2]
    planes, length = comp.shape[0], comp.shape[1]
    vmem = pl.BlockSpec(memory_space=pltpu.VMEM)
    hbm = pl.BlockSpec(memory_space=pltpu.HBM)
    message = (count, 4 * width + 8, LANES)
    return pl.pallas_call(
        functools.partial(spline_kernel, length ** (-0.5)),
        in_specs=[pl.BlockSpec(memory_space=pltpu.SMEM), vmem, vmem, vmem, hbm],
        out_specs=[hbm, vmem],
        out_shape=[pltpu.HBM(message, jnp.float32), jax.ShapeDtypeStruct((8, LANES), jnp.float32)],
        scratch_shapes=[
            pltpu.VMEM(message, jnp.float32),
            pltpu.VMEM((count, planes, width, LANES), jnp.float32),
            pltpu.SemaphoreType.DMA((count,)),
            pltpu.SemaphoreType.DMA((count,)),
        ],
        compiler_params=pltpu.CompilerParams(vmem_limit_bytes=28 * 1024 * 1024),
        name="splines",
    )(kernel_mesh, table, wave, kept, in_hbm(comp))


def edges_kernel(order_ref, density_ref, gradient_ref, push_ref, weight_ref, density, first, third, arrived):
    width, rows = density_ref.shape[0], density_ref.shape[1]
    copies = [
        pltpu.make_async_copy(density_ref, density, arrived.at[0]),
        pltpu.make_async_copy(gradient_ref.at[2], third, arrived.at[1]),
        pltpu.make_async_copy(gradient_ref.at[0, 0], first.at[0], arrived.at[2]),
        pltpu.make_async_copy(gradient_ref.at[0, width - 1], first.at[1], arrived.at[3]),
    ]
    for copy in copies:
        copy.start()
    for copy in copies:
        copy.wait()
    push_ref[0] = density[0] * first[0]
    push_ref[1] = density[width - 1] * first[1]
    lane = lax.broadcasted_iota(jnp.int32, (rows, LANES), 1)
    low = order_ref[:1] + jnp.zeros((rows, LANES), jnp.float32)
    high = low
    for x in range(width):
        product = density[x] * third[x]
        low = jnp.where(lane == x, product[:, :1], low)
        high = jnp.where(lane == x, product[:, LANES - 1 :], high)
    weight_ref[0] = low
    weight_ref[1] = high


def edges(order, density, gradient):
    rows = density.shape[1]
    vmem, hbm = pl.BlockSpec(memory_space=pltpu.VMEM), pl.BlockSpec(memory_space=pltpu.HBM)
    face = jax.ShapeDtypeStruct((2, rows, LANES), jnp.float32)
    return pl.pallas_call(
        edges_kernel,
        in_specs=[vmem, hbm, hbm],
        out_specs=[vmem, vmem],
        out_shape=[face, face],
        scratch_shapes=[
            pltpu.VMEM(density.shape, jnp.float32),
            pltpu.VMEM((2, rows, LANES), jnp.float32),
            pltpu.VMEM(density.shape, jnp.float32),
            pltpu.SemaphoreType.DMA((4,)),
        ],
        compiler_params=pltpu.CompilerParams(vmem_limit_bytes=8 * 1024 * 1024),
        name="edges",
    )(order, in_hbm(density), in_hbm(gradient))


def faces_kernel(width, got_ref, weight_ref, low_ref, high_ref):
    part, rows = 2 * width + 4, weight_ref.shape[1]
    for side, out_ref in enumerate((low_ref, high_ref)):
        out_ref[...] = got_ref[pl.ds(2 * width + 2 + side, rows, stride=part), :] * weight_ref[side]


def faces(got, weight, width):
    vmem = pl.BlockSpec(memory_space=pltpu.VMEM)
    return pl.pallas_call(
        functools.partial(faces_kernel, width),
        in_specs=[vmem, vmem],
        out_specs=[vmem, vmem],
        out_shape=[jax.ShapeDtypeStruct(weight.shape[1:], jnp.float32)] * 2,
        compiler_params=pltpu.CompilerParams(vmem_limit_bytes=8 * 1024 * 1024),
        name="faces",
    )(got, weight)


def inner_kernel(got_ref, push_ref, density_ref, rate_ref, gradient_ref, result, density, rate, gradient, arrived):
    width, rows = density_ref.shape[0], density_ref.shape[1]
    part = 2 * width + 4
    share = width // SLICES

    def copies(n):
        at = pl.ds(n * share, share)
        return [
            pltpu.make_async_copy(density_ref.at[at], density.at[at], arrived.at[n, 0]),
            pltpu.make_async_copy(rate_ref.at[at], rate.at[at], arrived.at[n, 1]),
            pltpu.make_async_copy(gradient_ref.at[:, at], gradient.at[:, at], arrived.at[n, 2]),
        ]

    for n in range(SLICES):
        for copy in copies(n):
            copy.start()

    def field(at):
        return got_ref[pl.ds(at, rows, stride=part), :]

    lane = lax.broadcasted_iota(jnp.int32, (rows, LANES), 1)
    ready = 0
    slope = [None] * width
    first = [None] * width
    for x in range(-1, width):
        ahead = x + 1
        if ahead < width:
            if ahead % share == 0:
                for copy in copies(ahead // share):
                    copy.wait()
            slope[ahead] = field(width + ahead) * density[ahead]
            first[ahead] = slope[ahead] * gradient[0, ahead]
        if x < 0:
            continue
        below = first[x - 1] if x > 0 else field(2 * width) * push_ref[0]
        above = first[x + 1] if x + 1 < width else field(2 * width + 1) * push_ref[1]
        second = slope[x] * gradient[1, x]
        third = slope[x] * gradient[2, x]
        beyond = jnp.where(lane == LANES - 1, 0.0, pltpu.roll(third, LANES - 1, 1))
        behind = jnp.where(lane == 0, 0.0, pltpu.roll(third, 1, 1))
        divergence = (above - below) + (beyond - behind)
        divergence = divergence + (pltpu.roll(second, rows - 1, 0) - pltpu.roll(second, 1, 0))
        result[x] = field(x) + rate[x] * slope[x] - 0.5 * divergence


def inner(got, push, density, rate, gradient):
    vmem, hbm = pl.BlockSpec(memory_space=pltpu.VMEM), pl.BlockSpec(memory_space=pltpu.HBM)
    return pl.pallas_call(
        inner_kernel,
        in_specs=[vmem, vmem, hbm, hbm, hbm],
        out_specs=vmem,
        out_shape=jax.ShapeDtypeStruct(density.shape, jnp.float32),
        scratch_shapes=[
            pltpu.VMEM(density.shape, jnp.float32),
            pltpu.VMEM(density.shape, jnp.float32),
            pltpu.VMEM(gradient.shape, jnp.float32),
            pltpu.SemaphoreType.DMA((SLICES, 3)),
        ],
        compiler_params=pltpu.CompilerParams(vmem_limit_bytes=16 * 1024 * 1024),
        name="inner",
    )(got, push, in_hbm(density), in_hbm(rate), in_hbm(gradient))


def outer_kernel(part_ref, low_ref, high_ref, out_hbm, out_ref, left):
    width, rows = part_ref.shape[0], part_ref.shape[1]
    share = width // SLICES
    lane = lax.broadcasted_iota(jnp.int32, (rows, LANES), 1)

    def store(n):
        at = pl.ds(n * share, share)
        return pltpu.make_async_copy(out_ref.at[at], out_hbm.at[at], left.at[n])

    for x in range(width):
        high = jnp.where(lane == LANES - 1, high_ref[:, x : x + 1], 0.0)
        flux = jnp.where(lane == 0, low_ref[:, x : x + 1], 0.0) - high
        out_ref[x] = part_ref[x] + 0.5 * flux
        if (x + 1) % share == 0:
            store(x // share).start()
    for n in range(SLICES):
        store(n).wait()


def outer(part, low, high):
    vmem, hbm = pl.BlockSpec(memory_space=pltpu.VMEM), pl.BlockSpec(memory_space=pltpu.HBM)
    return pl.pallas_call(
        outer_kernel,
        in_specs=[vmem] * 3,
        out_specs=hbm,
        out_shape=jax.ShapeDtypeStruct(part.shape, jnp.float32),
        scratch_shapes=[pltpu.VMEM(part.shape, jnp.float32), pltpu.SemaphoreType.DMA((SLICES,))],
        compiler_params=pltpu.CompilerParams(vmem_limit_bytes=8 * 1024 * 1024),
        name="outer",
    )(part, low, high)


def neighbours(axis):
    count = lax.axis_size(axis)
    forward = [(i, (i + 1) % count) for i in range(count)]
    return forward, [(target, source) for source, target in forward]


def turn_kernel(wave_ref, out_ref, held, arrived):
    width, rows = wave_ref.shape[0], wave_ref.shape[1]
    share = width // SLICES

    def copy(n):
        at = pl.ds(n * share, share)
        return pltpu.make_async_copy(wave_ref.at[at], held.at[at], arrived.at[n])

    for n in range(SLICES):
        copy(n).start()
    for x in range(width):
        if x % share == 0:
            copy(x // share).wait()
        out_ref[pl.ds(x, rows, stride=width), :] = held[x]


def turn(wave):
    width, rows = wave.shape[0], wave.shape[1]
    return pl.pallas_call(
        turn_kernel,
        in_specs=[pl.BlockSpec(memory_space=pltpu.HBM)],
        out_specs=pl.BlockSpec(memory_space=pltpu.VMEM),
        out_shape=pltpu.VMEM((rows * width, LANES), jnp.float32),
        scratch_shapes=[pltpu.VMEM(wave.shape, jnp.float32), pltpu.SemaphoreType.DMA((SLICES,))],
        compiler_params=pltpu.CompilerParams(vmem_limit_bytes=8 * 1024 * 1024),
        name="turn",
    )(in_hbm(wave))


def shards(spectra, kernel_mesh, density, local_wave, wave_density, wave_gradient):
    width, rows = density.shape[0], density.shape[1]
    count = lax.axis_size("gx")
    wave = turn(local_wave).reshape(count, 2, width, LANES)
    wave = lax.all_to_all(wave, "gx", 0, 0, tiled=True)
    comp, kept, table = transform(spectra, kernel_mesh)
    sent, order = splines(kernel_mesh, comp, kept, table, wave)
    got = lax.all_to_all(sent, "gx", 0, 0, tiled=True).reshape(-1, LANES)

    push, weight = edges(order, density, wave_gradient)
    forward, backward = neighbours("gx")
    push = jnp.concatenate(
        [lax.ppermute(push[1:], "gx", forward), lax.ppermute(push[:1], "gx", backward)], axis=0
    )
    forward, backward = neighbours("yz")
    got = pltpu.with_memory_space_constraint(got, pltpu.VMEM)
    third_low, third_high = faces(got, weight, width)
    low = lax.ppermute(third_high, "yz", forward)
    high = lax.ppermute(third_low, "yz", backward)
    part = inner(got, push, density, wave_density, wave_gradient)
    return outer(part, low, high)


def solution(mesh):
    return jax.shard_map(
        shards,
        mesh=mesh,
        in_specs=(
            P(None, None, None, "gx", "yz"),
            P(),
            P("gx", None, "yz"),
            P("gx", None, "yz"),
            P("gx", None, "yz"),
            P(None, "gx", None, "yz"),
        ),
        out_specs=P("gx", None, "yz"),
        check_vma=False,
    )
```

```python
import functools
import math

import jax
import jax.numpy as jnp
import numpy as np
from jax import lax
from jax.experimental import pallas as pl
from jax.experimental.pallas import tpu as pltpu
from jax.sharding import PartitionSpec as P

LANES = 128
POINTS = 20
KEPT = 4
GROUPS = (2, 4, 6, 4, 4)
SLICES = 4
AHEAD = 10
BLOCKS_AHEAD = 4
IH, LOW, INV, ROWS = 0, 20, 40, 60


def in_hbm(array):
    return pltpu.with_memory_space_constraint(array, pltpu.HBM)


def half_tables(length):
    half = length // 2
    cells = np.arange(half)[:, None]
    tables = []
    for parity in range(2):
        waves = 2 * np.arange(half)[None, :] + parity
        angles = 2.0 * math.pi * (waves * cells % length) / length
        tables.append(np.concatenate([np.cos(angles), -np.sin(angles)], axis=1))
    return np.stack(tables).astype(jnp.bfloat16)


def spline_table(mesh_ref, table_ref):
    tile = (8, LANES)
    mesh = [jnp.full(tile, mesh_ref[j], jnp.float32) for j in range(POINTS)]
    steps = [mesh[j + 1] - mesh[j] for j in range(POINTS - 1)]
    for j in range(POINTS - 1):
        table_ref[IH + j] = 1.0 / steps[j]
    low = jnp.zeros(tile, jnp.float32)
    for j in range(1, POINTS - 1):
        pivot = (steps[j - 1] + steps[j]) / 3.0 - low * (steps[j - 1] / 6.0)
        inverse = 1.0 / pivot
        table_ref[LOW + j] = low
        table_ref[INV + j] = inverse
        low = (steps[j] / 6.0) * inverse
    table_ref[LOW + POINTS - 1] = low


def transform_kernel(mesh_ref, tables_hbm, spectra_ref, comp_ref, kept_ref, table_ref, tables_ref, held, wide, done, arrived, left):
    length = comp_ref.shape[1]
    half = length // 2

    def copy(c):
        return pltpu.make_async_copy(spectra_ref.at[:, c], held.at[c], arrived.at[c])

    def store(start, size, slot):
        size = min(size, POINTS - KEPT - start)
        planes = pl.ds(2 * start, 2 * size)
        return pltpu.make_async_copy(done.at[slot, pl.ds(0, 2 * size)], comp_ref.at[planes], left.at[slot])

    tables_copy = pltpu.make_async_copy(tables_hbm, tables_ref, left.at[2])
    copy(0).start()
    tables_copy.start()
    for c in range(1, AHEAD):
        copy(c).start()
    spline_table(mesh_ref, table_ref)
    tables_copy.wait()

    starts = [sum(GROUPS[:g]) for g in range(len(GROUPS))]
    sent = [g for g in range(len(GROUPS)) if starts[g] < POINTS - KEPT]
    for g, (start, size) in enumerate(zip(starts, GROUPS)):
        slot = g % 2
        if g >= 2 and g in sent:
            store(starts[g - 2], GROUPS[g - 2], slot).wait()
        for c in range(start, start + size):
            copy(c).wait()
            if c + AHEAD < POINTS:
                copy(c + AHEAD).start()
        for i in range(size):
            c = start + i
            for p in range(2):
                wide[i, p] = held[c, p].astype(jnp.float32)
            parts = []
            for parity in range(2):
                operand = jnp.concatenate(
                    [
                        jnp.concatenate(
                            [
                                wide[i, p, pl.ds(2 * parity + y, half, stride=4), :].astype(jnp.bfloat16)
                                for y in range(2)
                            ],
                            axis=1,
                        )
                        for p in range(2)
                    ],
                    axis=0,
                )
                parts.append(jnp.dot(tables_ref[parity], operand, preferred_element_type=jnp.float32))
            total, difference = parts[0] + parts[1], parts[0] - parts[1]
            for y in range(2):
                if c < POINTS - KEPT:
                    plane = done.at[slot, 2 * i + y]
                else:
                    plane = kept_ref.at[2 * (c - POINTS + KEPT) + y]
                plane[:half, :] = total[:, y * LANES : (y + 1) * LANES]
                plane[half:, :] = difference[:, y * LANES : (y + 1) * LANES]
        if g in sent:
            store(start, size, slot).start()
    for g in sent[-2:]:
        store(starts[g], GROUPS[g], g % 2).wait()


def transform(spectra, kernel_mesh):
    comps, length = spectra.shape[1], spectra.shape[2]
    tables = jnp.asarray(half_tables(length))
    flat = spectra.reshape(2, comps, 2 * length, LANES)
    return pl.pallas_call(
        transform_kernel,
        in_specs=[
            pl.BlockSpec(memory_space=pltpu.SMEM),
            pl.BlockSpec(memory_space=pltpu.HBM),
            pl.BlockSpec(memory_space=pltpu.HBM),
        ],
        out_specs=[pl.BlockSpec(memory_space=pltpu.HBM)] + [pl.BlockSpec(memory_space=pltpu.VMEM)] * 2,
        out_shape=[
            pltpu.HBM((2 * (comps - KEPT), length, LANES), jnp.float32),
            jax.ShapeDtypeStruct((2 * KEPT, length, LANES), jnp.float32),
            jax.ShapeDtypeStruct((ROWS, 8, LANES), jnp.float32),
        ],
        scratch_shapes=[
            pltpu.VMEM((2, length // 2, length), jnp.bfloat16),
            pltpu.VMEM((comps, 2, 2 * length, LANES), jnp.bfloat16),
            pltpu.VMEM((max(GROUPS), 2, 2 * length, LANES), jnp.float32),
            pltpu.VMEM((2, 2 * max(GROUPS), length, LANES), jnp.float32),
            pltpu.SemaphoreType.DMA((comps,)),
            pltpu.SemaphoreType.DMA((3,)),
        ],
        compiler_params=pltpu.CompilerParams(vmem_limit_bytes=40 * 1024 * 1024),
        cost_estimate=pl.CostEstimate(
            flops=4 * comps * length * length * LANES,
            bytes_accessed=12 * comps * length * 2 * LANES,
            transcendentals=0,
        ),
        name="transform",
    )(kernel_mesh, in_hbm(tables), in_hbm(flat))


def solve(comp, table):
    before = (comp(1) - comp(0)) * table(IH)
    forward = [None] * POINTS
    for j in range(1, POINTS - 1):
        step = (comp(j + 1) - comp(j)) * table(IH + j)
        forward[j] = step - before
        if j > 1:
            forward[j] = forward[j] - table(LOW + j) * forward[j - 1]
        before = step
    second = [None] * POINTS
    for j in range(POINTS - 2, 0, -1):
        second[j] = forward[j] * table(INV + j)
        if j < POINTS - 2:
            second[j] = second[j] - table(LOW + j + 1) * second[j + 1]
    second[0] = second[POINTS - 1] = jnp.zeros_like(before)
    return second


def evaluate(comp, second, mesh, wave):
    top = wave >= mesh(16)

    def halve(nodes, past):
        half = len(nodes) // 2
        return [jnp.where(past, nodes[half + k], nodes[k]) for k in range(half + 1)]

    def spread(node):
        nodes = [node(k) for k in range(17)]
        return [jnp.where(top, node(16 + k), nodes[k]) for k in range(4)] + nodes[4:]

    nodes, turns = spread(mesh), []
    for half in (8, 4, 2, 1):
        past = wave >= nodes[half]
        if half >= 4:
            past = past & ~top
        if half == 1:
            past = past & (wave < mesh(POINTS - 2))
        turns.append(past)
        nodes = halve(nodes, past)
    low, high = nodes

    def pick(node):
        nodes = spread(node)
        for past in turns:
            nodes = halve(nodes, past)
        return nodes

    comp_low, comp_high = pick(comp)
    second_low, second_high = pick(second)
    width = high - low
    inverse = 1.0 / width
    a = (high - wave) * inverse
    b = (wave - low) * inverse
    sixth = width * (1.0 / 6.0)
    a2, b2 = a * a, b * b
    value = a * comp_low + b * comp_high + (
        (a2 - 1.0) * a * second_low + (b2 - 1.0) * b * second_high
    ) * (width * sixth)
    slope = (comp_high - comp_low) * inverse + (
        (3.0 * b2 - 1.0) * second_high - (3.0 * a2 - 1.0) * second_low
    ) * sixth
    return value, slope


def spline_kernel(scale, mesh_ref, table_ref, wave_ref, kept_ref, comp_ref, out_hbm, order_ref, out_ref, held, arrived, left):
    count, width = wave_ref.shape[0], wave_ref.shape[2]
    tiles = width // 8
    part = 2 * width + 4

    def copy(block):
        rows = pl.ds(pl.multiple_of(block * width, 8), width)
        return pltpu.make_async_copy(comp_ref.at[:, rows], held.at[block], arrived.at[block])

    def store(block):
        return pltpu.make_async_copy(out_ref.at[block], out_hbm.at[block], left.at[block])

    for block in range(BLOCKS_AHEAD):
        copy(block).start()
    order_ref[...] = jnp.zeros_like(order_ref)
    out_ref[count - 1] = jnp.zeros(out_ref.shape[1:], jnp.float32)
    mesh = [jnp.full((8, LANES), mesh_ref[j], jnp.float32) for j in range(POINTS)]

    def turn(block):
        slopes = [out_ref[block, y * part + width : y * part + 2 * width, :] for y in range(2)]
        slopes.append(jnp.zeros((LANES - 2 * width, LANES), jnp.float32))
        turned = jnp.concatenate(slopes, axis=0).T
        for side, edge in enumerate((turned[:1], turned[LANES - 1 :])):
            at = 2 * width + 2 + side
            out_ref[block, at : at + 1, :] = edge
            out_ref[block, part + at : part + at + 1, :] = pltpu.roll(edge, LANES - width, 1)

    def body(block, carry):
        following = lax.rem(block + 1, count)
        previous = lax.rem(block + count - 1, count)
        copy(block).wait()

        @pl.when(block + BLOCKS_AHEAD < count)
        def _():
            copy(block + BLOCKS_AHEAD).start()

        turn(previous)
        for y in range(2):
            wave = wave_ref[block, y].reshape(tiles, 8, LANES)

            def comp(j):
                if j < POINTS - KEPT:
                    return held[block, 2 * j + y].reshape(tiles, 8, LANES)
                rows = pl.ds(pl.multiple_of(block * width, 8), width)
                return kept_ref[2 * (j - POINTS + KEPT) + y, rows, :].reshape(tiles, 8, LANES)

            second = solve(comp, lambda j: table_ref[j])
            value, slope = evaluate(comp, lambda j: second[j], lambda j: mesh[j], wave)
            value = (value * scale).reshape(width, LANES)
            slope = (slope * scale).reshape(width, LANES)
            out_ref[block, y * part : y * part + width, :] = value
            out_ref[block, y * part + width : y * part + 2 * width, :] = slope
            at = y * part + 2 * width
            out_ref[following, at : at + 1, :] = slope[width - 1 :]
            out_ref[previous, at + 1 : at + 2, :] = slope[:1]
        @pl.when(block >= 2)
        def _():
            store(block - 1).start()

        return carry

    lax.fori_loop(0, count, body, 0)
    turn(count - 1)
    store(0).start()
    store(count - 1).start()
    for block in range(count):
        store(block).wait()


def splines(kernel_mesh, comp, kept, table, wave):
    count, width = wave.shape[0], wave.shape[2]
    planes, length = comp.shape[0], comp.shape[1]
    vmem = pl.BlockSpec(memory_space=pltpu.VMEM)
    hbm = pl.BlockSpec(memory_space=pltpu.HBM)
    message = (count, 4 * width + 8, LANES)
    return pl.pallas_call(
        functools.partial(spline_kernel, length ** (-0.5)),
        in_specs=[pl.BlockSpec(memory_space=pltpu.SMEM), vmem, vmem, vmem, hbm],
        out_specs=[hbm, vmem],
        out_shape=[pltpu.HBM(message, jnp.float32), jax.ShapeDtypeStruct((8, LANES), jnp.float32)],
        scratch_shapes=[
            pltpu.VMEM(message, jnp.float32),
            pltpu.VMEM((count, planes, width, LANES), jnp.float32),
            pltpu.SemaphoreType.DMA((count,)),
            pltpu.SemaphoreType.DMA((count,)),
        ],
        compiler_params=pltpu.CompilerParams(vmem_limit_bytes=28 * 1024 * 1024),
        name="splines",
    )(kernel_mesh, table, wave, kept, in_hbm(comp))


def edges_kernel(order_ref, density_ref, gradient_ref, push_ref, weight_ref, density, first, third, arrived):
    width, rows = density_ref.shape[0], density_ref.shape[1]
    copies = [
        pltpu.make_async_copy(density_ref, density, arrived.at[0]),
        pltpu.make_async_copy(gradient_ref.at[2], third, arrived.at[1]),
        pltpu.make_async_copy(gradient_ref.at[0, 0], first.at[0], arrived.at[2]),
        pltpu.make_async_copy(gradient_ref.at[0, width - 1], first.at[1], arrived.at[3]),
    ]
    for copy in copies:
        copy.start()
    for copy in copies:
        copy.wait()
    push_ref[0] = density[0] * first[0]
    push_ref[1] = density[width - 1] * first[1]
    lane = lax.broadcasted_iota(jnp.int32, (rows, LANES), 1)
    low = order_ref[:1] + jnp.zeros((rows, LANES), jnp.float32)
    high = low
    for x in range(width):
        product = density[x] * third[x]
        low = jnp.where(lane == x, product[:, :1], low)
        high = jnp.where(lane == x, product[:, LANES - 1 :], high)
    weight_ref[0] = low
    weight_ref[1] = high


def edges(order, density, gradient):
    rows = density.shape[1]
    vmem, hbm = pl.BlockSpec(memory_space=pltpu.VMEM), pl.BlockSpec(memory_space=pltpu.HBM)
    face = jax.ShapeDtypeStruct((2, rows, LANES), jnp.float32)
    return pl.pallas_call(
        edges_kernel,
        in_specs=[vmem, hbm, hbm],
        out_specs=[vmem, vmem],
        out_shape=[face, face],
        scratch_shapes=[
            pltpu.VMEM(density.shape, jnp.float32),
            pltpu.VMEM((2, rows, LANES), jnp.float32),
            pltpu.VMEM(density.shape, jnp.float32),
            pltpu.SemaphoreType.DMA((4,)),
        ],
        compiler_params=pltpu.CompilerParams(vmem_limit_bytes=8 * 1024 * 1024),
        name="edges",
    )(order, in_hbm(density), in_hbm(gradient))


def faces_kernel(width, got_ref, weight_ref, low_ref, high_ref):
    part, rows = 2 * width + 4, weight_ref.shape[1]
    for side, out_ref in enumerate((low_ref, high_ref)):
        out_ref[...] = got_ref[pl.ds(2 * width + 2 + side, rows, stride=part), :] * weight_ref[side]


def faces(got, weight, width):
    vmem = pl.BlockSpec(memory_space=pltpu.VMEM)
    return pl.pallas_call(
        functools.partial(faces_kernel, width),
        in_specs=[vmem, vmem],
        out_specs=[vmem, vmem],
        out_shape=[jax.ShapeDtypeStruct(weight.shape[1:], jnp.float32)] * 2,
        compiler_params=pltpu.CompilerParams(vmem_limit_bytes=8 * 1024 * 1024),
        name="faces",
    )(got, weight)


def inner_kernel(got_ref, push_ref, density_ref, rate_ref, gradient_ref, result, density, rate, gradient, arrived):
    width, rows = density_ref.shape[0], density_ref.shape[1]
    part = 2 * width + 4
    share = width // SLICES

    def copies(n):
        at = pl.ds(n * share, share)
        return [
            pltpu.make_async_copy(density_ref.at[at], density.at[at], arrived.at[n, 0]),
            pltpu.make_async_copy(rate_ref.at[at], rate.at[at], arrived.at[n, 1]),
            pltpu.make_async_copy(gradient_ref.at[:, at], gradient.at[:, at], arrived.at[n, 2]),
        ]

    for n in range(SLICES):
        for copy in copies(n):
            copy.start()

    def field(at):
        return got_ref[pl.ds(at, rows, stride=part), :]

    lane = lax.broadcasted_iota(jnp.int32, (rows, LANES), 1)
    ready = 0
    slope = [None] * width
    first = [None] * width
    for x in range(-1, width):
        ahead = x + 1
        if ahead < width:
            if ahead % share == 0:
                for copy in copies(ahead // share):
                    copy.wait()
            slope[ahead] = field(width + ahead) * density[ahead]
            first[ahead] = slope[ahead] * gradient[0, ahead]
        if x < 0:
            continue
        below = first[x - 1] if x > 0 else field(2 * width) * push_ref[0]
        above = first[x + 1] if x + 1 < width else field(2 * width + 1) * push_ref[1]
        second = slope[x] * gradient[1, x]
        third = slope[x] * gradient[2, x]
        beyond = jnp.where(lane == LANES - 1, 0.0, pltpu.roll(third, LANES - 1, 1))
        behind = jnp.where(lane == 0, 0.0, pltpu.roll(third, 1, 1))
        divergence = (above - below) + (beyond - behind)
        divergence = divergence + (pltpu.roll(second, rows - 1, 0) - pltpu.roll(second, 1, 0))
        result[x] = field(x) + rate[x] * slope[x] - 0.5 * divergence


def inner(got, push, density, rate, gradient):
    vmem, hbm = pl.BlockSpec(memory_space=pltpu.VMEM), pl.BlockSpec(memory_space=pltpu.HBM)
    return pl.pallas_call(
        inner_kernel,
        in_specs=[vmem, vmem, pl.BlockSpec(memory_space=pl.ANY), pl.BlockSpec(memory_space=pl.ANY), hbm],
        out_specs=vmem,
        out_shape=jax.ShapeDtypeStruct(density.shape, jnp.float32),
        scratch_shapes=[
            pltpu.VMEM(density.shape, jnp.float32),
            pltpu.VMEM(density.shape, jnp.float32),
            pltpu.VMEM(gradient.shape, jnp.float32),
            pltpu.SemaphoreType.DMA((SLICES, 3)),
        ],
        compiler_params=pltpu.CompilerParams(vmem_limit_bytes=16 * 1024 * 1024),
        name="inner",
    )(got, push, density, rate, in_hbm(gradient))


def outer_kernel(part_ref, low_ref, high_ref, out_hbm, out_ref, left):
    width, rows = part_ref.shape[0], part_ref.shape[1]
    share = width // SLICES
    lane = lax.broadcasted_iota(jnp.int32, (rows, LANES), 1)

    def store(n):
        at = pl.ds(n * share, share)
        return pltpu.make_async_copy(out_ref.at[at], out_hbm.at[at], left.at[n])

    for x in range(width):
        high = jnp.where(lane == LANES - 1, high_ref[:, x : x + 1], 0.0)
        flux = jnp.where(lane == 0, low_ref[:, x : x + 1], 0.0) - high
        out_ref[x] = part_ref[x] + 0.5 * flux
        if (x + 1) % share == 0:
            store(x // share).start()
    for n in range(SLICES):
        store(n).wait()


def outer(part, low, high):
    vmem, hbm = pl.BlockSpec(memory_space=pltpu.VMEM), pl.BlockSpec(memory_space=pltpu.HBM)
    return pl.pallas_call(
        outer_kernel,
        in_specs=[vmem] * 3,
        out_specs=hbm,
        out_shape=jax.ShapeDtypeStruct(part.shape, jnp.float32),
        scratch_shapes=[pltpu.VMEM(part.shape, jnp.float32), pltpu.SemaphoreType.DMA((SLICES,))],
        compiler_params=pltpu.CompilerParams(vmem_limit_bytes=8 * 1024 * 1024),
        name="outer",
    )(part, low, high)


def neighbours(axis):
    count = lax.axis_size(axis)
    forward = [(i, (i + 1) % count) for i in range(count)]
    return forward, [(target, source) for source, target in forward]


def turn_kernel(wave_ref, out_ref, held, arrived):
    width, rows = wave_ref.shape[0], wave_ref.shape[1]
    share = width // SLICES

    def copy(n):
        at = pl.ds(n * share, share)
        return pltpu.make_async_copy(wave_ref.at[at], held.at[at], arrived.at[n])

    for n in range(SLICES):
        copy(n).start()
    for x in range(width):
        if x % share == 0:
            copy(x // share).wait()
        out_ref[pl.ds(x, rows, stride=width), :] = held[x]


def turn(wave):
    width, rows = wave.shape[0], wave.shape[1]
    return pl.pallas_call(
        turn_kernel,
        in_specs=[pl.BlockSpec(memory_space=pltpu.HBM)],
        out_specs=pl.BlockSpec(memory_space=pltpu.VMEM),
        out_shape=pltpu.VMEM((rows * width, LANES), jnp.float32),
        scratch_shapes=[pltpu.VMEM(wave.shape, jnp.float32), pltpu.SemaphoreType.DMA((SLICES,))],
        compiler_params=pltpu.CompilerParams(vmem_limit_bytes=8 * 1024 * 1024),
        name="turn",
    )(in_hbm(wave))


def shards(spectra, kernel_mesh, density, local_wave, wave_density, wave_gradient):
    width, rows = density.shape[0], density.shape[1]
    count = lax.axis_size("gx")
    wave = turn(local_wave).reshape(count, 2, width, LANES)
    wave = lax.all_to_all(wave, "gx", 0, 0, tiled=True)
    comp, kept, table = transform(spectra, kernel_mesh)
    sent, order = splines(kernel_mesh, comp, kept, table, wave)
    got = lax.all_to_all(sent, "gx", 0, 0, tiled=True).reshape(-1, LANES)

    push, weight = edges(order, density, wave_gradient)
    forward, backward = neighbours("gx")
    push = jnp.concatenate(
        [lax.ppermute(push[1:], "gx", forward), lax.ppermute(push[:1], "gx", backward)], axis=0
    )
    forward, backward = neighbours("yz")
    got = pltpu.with_memory_space_constraint(got, pltpu.VMEM)
    third_low, third_high = faces(got, weight, width)
    low = lax.ppermute(third_high, "yz", forward)
    high = lax.ppermute(third_low, "yz", backward)
    part = inner(got, push, density, wave_density, wave_gradient)
    return outer(part, low, high)


def solution(mesh):
    return jax.shard_map(
        shards,
        mesh=mesh,
        in_specs=(
            P(None, None, None, "gx", "yz"),
            P(),
            P("gx", None, "yz"),
            P("gx", None, "yz"),
            P("gx", None, "yz"),
            P(None, "gx", None, "yz"),
        ),
        out_specs=P("gx", None, "yz"),
        check_vma=False,
    )
```
